32 devices in a mesh: src: 16 (over z, y, core), sub: 2 (over x).
Axes of the slice: x: 2, y: 2, z: 4, core: 2. Of those that a mesh axis runs over, the one named last changes fastest.
Arguments:
- child_rhs: float32 [2, 1024, 4096], P('sub', None, 'src'), may hold values from -6 to 6
- root_rhs: float32 [2048, 4096], P('sub', 'src'), may hold values from -6 to 6
- child_inverse: bfloat16 [2, 1024, 1024], P('sub', 'src'), as said below
- coupling_block: bfloat16 [2, 1024, 1024], P('sub', 'src'), may hold values from -0.1875 to 0.1875
- root_inverse: bfloat16 [2048, 2048], P('sub', 'src'), as said below
- child_orders: int32 [2], P('sub'), may hold values from 716 to 1024, as said below
- coupling_rows: int32 [2, 1024], P('sub'), may hold values from 0 to 2047, as said below
Outputs:
- child_solution: float32 [2, 1024, 4096], P('sub', None, 'src')
- root_solution: float32 [2048, 4096], P('sub', 'src')
The draws below stay inside these ranges and needn't reach their ends.
Inputs may be any that keep to these rules, and one draw needn't show every extreme that they name: Each child_inverse[j] is lower triangular: zero above the diagonal, diagonal entries between 0.8 and 1.25. `root_inverse`: lower triangular: zero above the diagonal, diagonal entries between 0.8 and 1.25. `coupling_rows`: each row holds 1024 distinct root rows in increasing order. `child_orders`: some child has order 1024.
All inputs are finite; a program needn't handle non-finite values.
Results may differ from the reference program's by a relative error of at most 0.0093.
Values may be sent and summed in bfloat16 or wider, within the bound.
A program may use at most 64 MiB of HBM per device.

```python
import math
import jax
import jax.numpy as jnp

S0 = 2048
S1 = 1024
K = 1024
CHILDREN = 2
SOURCES = 4096


def lower_factor(key, batch_count, matrix_order):
    key_off, key_diag = jax.random.split(key)
    spread = jnp.clip(jax.random.normal(key_off, (batch_count, matrix_order, matrix_order), jnp.float32), -6.0, 6.0)
    diagonal = jax.random.uniform(key_diag, (batch_count, matrix_order), jnp.float32, 0.8, 1.25)
    positions = jnp.arange(matrix_order)
    strict_lower = positions[:, None] > positions[None, :]
    on_diagonal = positions[:, None] == positions[None, :]
    factor = jnp.where(strict_lower, spread * (0.5 / math.sqrt(matrix_order)), 0.0)
    return factor + jnp.where(on_diagonal, diagonal[:, :, None], 0.0)


def draw_child_inverse(key, part):
    return lower_factor(jax.random.fold_in(key, 11), CHILDREN, S1).astype(jnp.bfloat16)


def draw_root_inverse(key, part):
    return lower_factor(jax.random.fold_in(key, 12), 1, S0)[0].astype(jnp.bfloat16)


def draw_coupling_rows(key, part):

    def choose_rows(child_number):
        shuffled = jax.random.permutation(jax.random.fold_in(jax.random.fold_in(key, 13), child_number), S0)
        return jnp.sort(shuffled[:K])
    return jax.vmap(choose_rows)(jnp.arange(CHILDREN)).astype(jnp.int32)


def draw_child_orders(key, part):
    orders = jax.random.randint(jax.random.fold_in(key, 14), (CHILDREN,), 7 * S1 // 10, S1 + 1, jnp.int32)
    largest = jax.random.randint(jax.random.fold_in(key, 15), (), 0, CHILDREN, jnp.int32)
    return jnp.where(jnp.arange(CHILDREN, dtype=jnp.int32) == largest, S1, orders).astype(jnp.int32)


def block_levels(rng, extent, cuts, smallest, high):
    def one(dim, shards_of):
        heights = jax.random.uniform(jax.random.fold_in(jax.random.fold_in(rng, 6), dim), (shards_of,), jnp.float32, smallest / len(cuts), high / len(cuts))
        return jnp.repeat(jnp.exp(heights), extent[dim] // shards_of).reshape((-1,) + (1,) * (len(extent) - dim - 1))

    loudness = one(*cuts[0])
    for cut in cuts[1:]:
        loudness = loudness * one(*cut)
    return loudness


def bell_draw(stream_key, shape, scale, limit, shards=(), held_as=jnp.bfloat16):
    values = scale * jax.random.normal(stream_key, shape, jnp.float32)
    if shards:
        values = values * block_levels(stream_key, shape, shards, -0.22, 0.18)
    return jnp.clip(values, -limit, limit).astype(held_as)


def setup_inputs(seed: int = 0) -> dict:
    keys = jax.random.split(jax.random.key(seed), 8)
    return {
        "child_rhs": bell_draw(keys[0], (CHILDREN, S1, SOURCES), 1.0, 6.0, ((0, 2), (2, 16)), jnp.float32),
        "root_rhs": bell_draw(keys[1], (S0, SOURCES), 1.0, 6.0, ((0, 2), (1, 16)), jnp.float32),
        "child_inverse": draw_child_inverse(jax.random.fold_in(keys[7], 71), 0),
        "coupling_block": bell_draw(keys[3], (CHILDREN, K, S1), S1 ** -0.5, 0.1875, ((0, 2), (1, 16))),
        "root_inverse": draw_root_inverse(jax.random.fold_in(keys[7], 71), 0),
        "child_orders": draw_child_orders(jax.random.fold_in(keys[7], 71), 0),
        "coupling_rows": draw_coupling_rows(jax.random.fold_in(keys[7], 71), 0),
    }


def reference(child_rhs, root_rhs, child_inverse, coupling_block, root_inverse, child_orders, coupling_rows):
    positions = jnp.arange(S1, dtype=jnp.int32)
    update_total = jnp.zeros(root_rhs.shape, jnp.float32)
    solved_list = []
    for child in range(CHILDREN):
        alive = (positions < child_orders[child])[:, None]
        child_source = jnp.where(alive, child_rhs[child], 0.0).astype(jnp.bfloat16)
        solved = jnp.where(alive, jnp.dot(child_inverse[child], child_source, preferred_element_type=jnp.float32), 0.0)
        solved_list.append(solved)
        update = jnp.dot(coupling_block[child], solved.astype(jnp.bfloat16), preferred_element_type=jnp.float32)
        update_total = update_total.at[coupling_rows[child]].add(update)
    root_source = (root_rhs - update_total).astype(jnp.bfloat16)
    root_forward = jnp.dot(root_inverse, root_source, preferred_element_type=jnp.float32)
    root_round = root_forward.astype(jnp.bfloat16)
    root_solution = jnp.dot(root_inverse.T, root_round, preferred_element_type=jnp.float32)
    root_half = root_solution.astype(jnp.bfloat16)
    result_list = []
    for child in range(CHILDREN):
        alive = (positions < child_orders[child])[:, None]
        picked = root_half[coupling_rows[child]]
        pulled = jnp.dot(coupling_block[child].T, picked, preferred_element_type=jnp.float32)
        residue = jnp.where(alive, solved_list[child] - pulled, 0.0).astype(jnp.bfloat16)
        result = jnp.dot(child_inverse[child].T, residue, preferred_element_type=jnp.float32)
        result_list.append(jnp.where(alive, result, 0.0))
    return jnp.stack(result_list), root_solution
```

```python
import functools
import jax
import jax.numpy as jnp
from jax import lax
from jax.experimental import pallas as pl
from jax.experimental.pallas import tpu as pltpu
from jax.sharding import PartitionSpec as P

MESH = pl.DeviceIdType.MESH
F32 = jnp.float32
BF16 = jnp.bfloat16

INV, CPL, LAST, B2, B1, B0, CROSS = range(7)


def dot_t(left, right):
    return lax.dot_general(left, right, (((1,), (1,)), ((), ())), preferred_element_type=F32)


def dot_n(left, right):
    return jnp.dot(left, right, preferred_element_type=F32)


def kernel(
    lines, rhs_any, rrhs_any, inv_ref, cpl_ref, rinv_ref, order_ref, rows_ref, child_out, root_out,
    inv, cpl, root, hot, hott, column, rows_peer, rhs_ref, rrhs_ref,
    src_t, solved_t, upd_t, upd_peer, rr_give, rr_take, base_t, take, rr_t, sol_t, sol_b, res_t,
    recv, send_z, send_y, send_x, send_c, early_s, rows_r, rr_r, up_s, up_r, bk_s, bk_r, lay,
):
    me, x = lax.axis_index("src"), lax.axis_index("sub")
    core, y, z = me % 2, (me // 2) % 2, me // 4
    strip = inv_ref.shape[0]
    order = inv_ref.shape[1]
    width = rinv_ref.shape[1]
    part = root.shape[1]
    chunks = root.shape[0]
    per = rinv_ref.shape[0] // part
    block = 2 * part
    cols = rhs_ref.shape[1]
    hcols = cols // 2
    own_rows = rrhs_ref.shape[0]
    here = pl.multiple_of(x * hcols, hcols)
    there = pl.multiple_of((1 - x) * hcols, hcols)

    def src_of(zz, yy, cc):
        return (zz * 2 + yy) * 2 + cc

    def dev(zz, yy, cc, xx):
        return {"src": src_of(zz, yy, cc), "sub": xx}

    loads = [
        pltpu.make_async_copy(rhs_any, rhs_ref, lay.at[0]),
        pltpu.make_async_copy(rrhs_any, rrhs_ref, lay.at[1]),
    ]
    for copy in loads:
        copy.start()

    barrier = pltpu.get_barrier_semaphore()

    def hello(device):
        pl.semaphore_signal(barrier, inc=1, device_id=device, device_id_type=MESH)

    hello(dev(z, 1 - y, core, x))
    hello(dev(z, y, 1 - core, x))
    hello(dev(z, y, core, 1 - x))

    @pl.when(z > 0)
    def _():
        hello(dev(z - 1, y, core, x))

    @pl.when(z < lines - 1)
    def _():
        hello(dev(z + 1, y, core, x))

    def strip_ref(which, s):
        r = pl.multiple_of(s * strip, strip)
        return (inv if which == INV else cpl).at[pl.ds(r, strip), :]

    def cols_of(s):
        return pl.ds(pl.multiple_of(s * width, width), width)

    def chunk_ref(k, s):
        return root.at[k, :, cols_of(s)]

    placing = [
        pltpu.make_async_copy(inv_ref, strip_ref(INV, me), lay.at[2]),
        pltpu.make_async_copy(cpl_ref, strip_ref(CPL, me), lay.at[3]),
    ] + [
        pltpu.make_async_copy(
            rinv_ref.at[pl.ds(i * part, part), :], chunk_ref(per * x + i, me), lay.at[4 + i]
        )
        for i in range(per)
    ]
    for copy in placing:
        copy.start()

    last = chunks - 2 + x
    cross = chunks - 1 - x
    native_of = {B2: x == 1, B1: x == 0, B0: x == 0, LAST: x == 1}
    block_of = {B2: 2, B1: 1, B0: 0}

    def views(which, s):
        if which == INV:
            r = pl.multiple_of(s * strip, strip)
            return [
                (s * strip // part == q, inv.at[pl.ds(r, strip), pl.ds(0, (q + 1) * part)])
                for q in range(order // part)
            ]
        if which == CPL:
            return [(None, strip_ref(CPL, s))]
        if which in (LAST, CROSS):
            k = last if which == LAST else cross
            return [(s * width < (k + 1) * part, chunk_ref(k, s))]
        b = block_of[which]
        full = s * width < b * block + part
        some = jnp.logical_and(s * width >= b * block + part, s * width < (b + 1) * block)
        return [
            (full, root.at[pl.ds(2 * b, 2), :, cols_of(s)]),
            (some, chunk_ref(2 * b + 1, s)),
        ]

    def under(cond, f):
        if cond is None:
            f()
        else:
            pl.when(cond)(f)

    def rsem(which, s):
        if which == LAST:
            return recv.at[LAST + x, s]
        if which == CROSS:
            return recv.at[LAST + 1 - x, s]
        return recv.at[which if which < LAST else which + 1, s]

    def push(which, s, sem, device, wait=False):
        for cond, ref in views(which, s):
            def f(ref=ref):
                cp = pltpu.make_async_remote_copy(
                    src_ref=ref, dst_ref=ref, send_sem=sem, recv_sem=rsem(which, s),
                    device_id=device, device_id_type=MESH,
                )
                if wait:
                    cp.wait_send()
                else:
                    cp.start()
            under(cond, f)

    def arrive(which, s):
        for cond, ref in views(which, s):
            def f(ref=ref):
                pltpu.make_async_remote_copy(
                    src_ref=ref, dst_ref=ref, send_sem=recv.at[0, 0], recv_sem=rsem(which, s),
                    device_id=dev(z, y, 1 - core, x), device_id_type=MESH,
                ).wait_recv()
            under(cond, f)

    other = dev(z, y, core, 1 - x)

    def sends(which, zz, far, wait, mine=False):
        yy = 1 - y if far else y
        s = src_of(zz, yy, core)
        if not far:
            @pl.when(jnp.logical_and(zz <= z, z < lines - 1))
            def _():
                push(which, s, send_z.at[which, 0, zz], dev(z + 1, y, core, x), wait)

            @pl.when(jnp.logical_and(zz >= z, z > 0))
            def _():
                push(which, s, send_z.at[which, 1, zz], dev(z - 1, y, core, x), wait)

            push(which, s, send_y.at[which, zz], dev(z, 1 - y, core, x), wait)
        if which == LAST:
            wanted = jnp.logical_or(zz != z, x == 1) if not far else None
            under(wanted, lambda: push(which, s, send_x.at[int(far), zz], other, wait))
        push(which, s, send_c.at[which, int(far), zz], dev(z, y, 1 - core, x), wait)

    def own(which):
        if which in native_of:
            pl.when(jnp.logical_not(native_of[which]))(lambda: arrive(which, me))
        sends(which, z, False, False)

    def near(which, first=1, stop=None):
        def step(k, _):
            zz = z + ((k + 1) // 2) * (1 - 2 * (k % 2))

            @pl.when(jnp.logical_and(zz >= 0, zz < lines))
            def _():
                arrive(which, src_of(zz, y, core))
                sends(which, zz, False, False)
            return 0
        lax.fori_loop(first, 2 * lines - 1 if stop is None else stop, step, 0)

    def far(which):
        def step(k, _):
            zz = z + ((k + 1) // 2) * (1 - 2 * (k % 2))

            @pl.when(jnp.logical_and(zz >= 0, zz < lines))
            def _():
                arrive(which, src_of(zz, 1 - y, core))
                sends(which, zz, True, False)
            return 0
        lax.fori_loop(0, 2 * lines - 1, step, 0)

    def over_core(which):
        def step(k, _):
            arrive(which, src_of(k // 2, k % 2, 1 - core))
            return 0
        lax.fori_loop(0, 2 * lines, step, 0)

    def crossed():
        def step(k, _):
            s = src_of(k // 2, k % 2, core)

            @pl.when(jnp.logical_or(s != me, x == 0))
            def _():
                arrive(CROSS, s)
                push(CROSS, s, send_c.at[CROSS, k % 2, k // 2], dev(z, y, 1 - core, x))
            return 0
        lax.fori_loop(0, 2 * lines, step, 0)

    def cross_own(wait):
        @pl.when(x == 1)
        def _():
            push(CROSS, me, send_c.at[CROSS, y, z], dev(z, y, 1 - core, x), wait)

    def early(wait):
        def one(which, i):
            push(which, me, early_s.at[i], other, wait)

        @pl.when(x == 1)
        def _():
            one(CROSS, 0)
            one(B2, 1)

        @pl.when(x == 0)
        def _():
            one(B1, 2)
            one(B0, 3)

    def copy_rows():
        return pltpu.make_async_remote_copy(
            src_ref=rows_ref, dst_ref=rows_peer, send_sem=early_s.at[4], recv_sem=rows_r,
            device_id=other, device_id_type=MESH,
        )

    def copy_rrhs():
        return pltpu.make_async_remote_copy(
            src_ref=rr_give, dst_ref=rr_take, send_sem=early_s.at[5], recv_sem=rr_r,
            device_id=other, device_id_type=MESH,
        )

    def copy_update():
        return pltpu.make_async_remote_copy(
            src_ref=upd_t.at[pl.ds(there, hcols), :], dst_ref=upd_peer, send_sem=up_s,
            recv_sem=up_r, device_id=other, device_id_type=MESH,
        )

    def back(a):
        piece = sol_b.at[pl.ds(here, hcols), pl.ds(a * block, block)]
        return pltpu.make_async_remote_copy(
            src_ref=piece, dst_ref=piece, send_sem=bk_s.at[a], recv_sem=bk_r.at[a],
            device_id=other, device_id_type=MESH,
        )

    def turn(slot, index):
        column[slot] = jnp.broadcast_to(index, (width, order)).T

    def scatter_ones(slot):
        @pl.loop(0, order // width)
        def _(i):
            r = pl.multiple_of(i * width, width)
            at = column[slot, pl.ds(r, width), :]
            lane = lax.broadcasted_iota(jnp.int32, (width, width), 1)
            for t in range(hott.shape[2] // width):
                hott[slot, pl.ds(r, width), pl.ds(t * width, width)] = jnp.where(
                    at == lane + t * width, 1.0, 0.0
                ).astype(BF16)

    def gather_ones(index):
        @pl.loop(0, hot.shape[0] // part)
        def _(i):
            r = pl.multiple_of(i * part, part)
            at = lax.broadcasted_iota(jnp.int32, (part, order), 0) + r
            hot[pl.ds(r, part), :] = jnp.where(at == index, 1.0, 0.0).astype(BF16)

    inner = jnp.logical_and(z > 0, z < lines - 1)
    pl.when(inner)(lambda: pl.semaphore_wait(barrier, 5))
    pl.when(jnp.logical_not(inner))(lambda: pl.semaphore_wait(barrier, 4))
    for copy in placing:
        copy.wait()

    own(INV)
    early(False)
    copy_rows().start()
    pl.when(x == 1)(lambda: own(LAST))
    own(CPL)
    cross_own(False)
    for copy in loads:
        copy.wait()
    rr_give[...] = rrhs_ref[:, pl.ds(there, hcols)].T.astype(BF16)
    copy_rrhs().start()
    pl.when(x == 0)(lambda: own(LAST))
    near(INV)
    near(LAST)
    alive = lax.broadcasted_iota(jnp.int32, (1, order), 1) < order_ref[0]
    src_t[...] = jnp.where(alive, rhs_ref[...].T, 0.0).astype(BF16)
    near(CPL)
    far(INV)
    index = rows_ref[...]
    turn(0, index)
    scatter_ones(0)
    own(B2)
    far(LAST)
    near(B2)
    over_core(INV)
    for q in range(order // part):
        at = pl.ds(q * part, part)
        upto = pl.ds(0, (q + 1) * part)
        solved_t[:, at] = jnp.where(
            alive[:, q * part:(q + 1) * part], dot_t(src_t[:, upto], inv[at, upto]), 0.0
        )
    own(B1)
    own(B0)
    far(CPL)
    near(B1)
    near(B0)
    over_core(CPL)
    upd_t[...] = dot_t(solved_t[...].astype(BF16), cpl[...]).astype(BF16)
    copy_update().start()
    far(B2)
    crossed()
    mine = pl.ds(pl.multiple_of(x * own_rows, own_rows), own_rows)
    theirs = pl.ds(pl.multiple_of((1 - x) * own_rows, own_rows), own_rows)
    copy_rrhs().wait_recv()
    base_t[:, mine] = rrhs_ref[:, pl.ds(here, hcols)].T
    base_t[:, theirs] = rr_take[...].astype(F32)
    mine_upd = upd_t[pl.ds(here, hcols), :]
    for i in range(hott.shape[2] // block):
        at = pl.ds(i * block, block)
        base_t[:, at] = base_t[:, at] - dot_n(mine_upd, hott[0, :, at])
    copy_rows().wait_recv()
    turn(1, rows_peer[...])
    scatter_ones(1)
    far(B1)
    far(B0)
    gather_ones(index)
    over_core(LAST)
    over_core(CROSS)
    copy_update().wait_recv()
    for i in range(hott.shape[2] // block):
        at = pl.ds(i * block, block)
        take[:, at] = (base_t[:, at] - dot_n(upd_peer[...], hott[1, :, at])).astype(BF16)

    blocks = chunks // 2
    for b in reversed(range(blocks)):
        if b < blocks - 1:
            over_core((B0, B1, B2)[b])
        for k in (2 * b + 1, 2 * b):
            upto = pl.ds(0, (k + 1) * part)
            rr_t[:, pl.ds(k * part, part)] = dot_t(take[:, upto], root[k, :, upto]).astype(BF16)
        low, high = 2 * b, 2 * b + 1
        r_low, r_high = rr_t[:, pl.ds(low * part, part)], rr_t[:, pl.ds(high * part, part)]
        at_low, at_high = pl.ds(low * part, part), pl.ds(high * part, part)
        s_low = dot_n(r_low, root[low, :, at_low]) + dot_n(r_high, root[high, :, at_low])
        s_high = dot_n(r_high, root[high, :, at_high])
        if b < blocks - 1:
            s_low += sol_t[:, at_low]
            s_high += sol_t[:, at_high]
        sol_t[:, at_low] = s_low
        sol_t[:, at_high] = s_high
        sol_b[pl.ds(here, hcols), at_low] = s_low.astype(BF16)
        sol_b[pl.ds(here, hcols), at_high] = s_high.astype(BF16)
        if b < blocks - 1:
            back(b + 1).start()
        for a in reversed(range(b)):
            at = pl.ds(a * block, block)
            more = dot_n(r_low, root[low, :, at]) + dot_n(r_high, root[high, :, at])
            sol_t[:, at] = more if b == blocks - 1 else sol_t[:, at] + more
    back(0).start()

    def finish(first, picked):
        rows = pl.ds(first, hcols)
        pulled = dot_n(picked.astype(BF16), cpl[...])
        res_t[...] = jnp.where(alive, solved_t[rows, :] - pulled, 0.0).astype(BF16)
        for q in range(order // part):
            at, rest = pl.ds(q * part, part), pl.ds(q * part, order - q * part)
            solved = jnp.where(
                alive[:, q * part:(q + 1) * part], dot_n(res_t[:, rest], inv[rest, at]), 0.0
            )
            child_out[at, rows] = solved.T

    finish(here, dot_n(sol_b[pl.ds(here, hcols), :], hot[...]))
    root_out[:, pl.ds(here, hcols)] = sol_t[:, mine].T
    for a in range(1, blocks):
        back(a).wait_recv()
    upper = pl.ds(block, (blocks - 1) * block)
    picked = dot_n(sol_b[pl.ds(there, hcols), upper], hot[upper, :])
    back(0).wait_recv()
    lower = pl.ds(0, block)
    picked += dot_n(sol_b[pl.ds(there, hcols), lower], hot[lower, :])
    finish(there, picked)
    root_out[:, pl.ds(there, hcols)] = sol_b[pl.ds(there, hcols), mine].astype(F32).T

    early(True)
    cross_own(True)
    copy_rows().wait_send()
    copy_rrhs().wait_send()
    copy_update().wait_send()
    for a in range(blocks):
        back(a).wait_send()
    for which in (INV, CPL, LAST, B2, B1, B0):
        for away in (False, True):
            def step(zz, _, which=which, away=away):
                sends(which, zz, away, True)
                return 0
            lax.fori_loop(0, lines, step, 0)

    def step(k, _):
        s = src_of(k // 2, k % 2, core)

        @pl.when(jnp.logical_or(s != me, x == 0))
        def _():
            push(CROSS, s, send_c.at[CROSS, k % 2, k // 2], dev(z, y, 1 - core, x), True)
        return 0
    lax.fori_loop(0, 2 * lines, step, 0)


def fused(child_rhs, root_rhs, child_inverse, coupling_block, root_inverse, child_orders, coupling_rows):
    n = lax.axis_size("src")
    lines = n // 4
    order = child_inverse.shape[2]
    cols = child_rhs.shape[2]
    own_rows = root_rhs.shape[0]
    root_order = own_rows * lax.axis_size("sub")
    couples = coupling_block.shape[1] * n
    part = root_order // 8
    width = root_inverse.shape[1]
    half = cols // 2
    vmem = pl.BlockSpec(memory_space=pltpu.VMEM)
    smem = pl.BlockSpec(memory_space=pltpu.SMEM)
    anywhere = pl.BlockSpec(memory_space=pl.ANY)
    dma = pltpu.SemaphoreType.DMA
    child_out, root_out = pl.pallas_call(
        functools.partial(kernel, lines),
        out_shape=(
            jax.ShapeDtypeStruct((order, cols), F32),
            jax.ShapeDtypeStruct((own_rows, cols), F32),
        ),
        in_specs=[anywhere] * 2 + [vmem] * 3 + [smem, vmem],
        out_specs=(vmem, vmem),
        scratch_shapes=[
            pltpu.VMEM((order, order), BF16),
            pltpu.VMEM((couples, order), BF16),
            pltpu.VMEM((8, part, root_order), BF16),
            pltpu.VMEM((root_order, couples), BF16),
            pltpu.VMEM((2, couples, root_order), BF16),
            pltpu.VMEM((2, couples, width), jnp.int32),
            pltpu.VMEM((1, couples), jnp.int32),
            pltpu.VMEM((order, cols), F32),
            pltpu.VMEM((own_rows, cols), F32),
            pltpu.VMEM((cols, order), BF16),
            pltpu.VMEM((cols, order), F32),
            pltpu.VMEM((cols, couples), BF16),
            pltpu.VMEM((half, couples), BF16),
            pltpu.VMEM((half, own_rows), BF16),
            pltpu.VMEM((half, own_rows), BF16),
            pltpu.VMEM((half, root_order), F32),
            pltpu.VMEM((half, root_order), BF16),
            pltpu.VMEM((half, root_order), BF16),
            pltpu.VMEM((half, root_order), F32),
            pltpu.VMEM((cols, root_order), BF16),
            pltpu.VMEM((half, order), BF16),
            dma((7, n)),
            dma((6, 2, lines)),
            dma((6, lines)),
            dma((2, lines)),
            dma((7, 2, lines)),
            dma((6,)),
            dma,
            dma,
            dma,
            dma,
            dma((4,)),
            dma((4,)),
            dma((8,)),
        ],
        compiler_params=pltpu.CompilerParams(
            collective_id=0, has_side_effects=True, vmem_limit_bytes=60 * 1024 * 1024
        ),
    )(child_rhs[0], root_rhs, child_inverse[0], coupling_block[0], root_inverse, child_orders, coupling_rows)
    return child_out[None], root_out


def contract_rows(left, right):
    return lax.dot_general(
        left, right, (((0,), (0,)), ((), ())), preferred_element_type=jnp.float32
    )


def on_device(
    child_rhs, root_rhs, child_inverse, coupling_block, root_inverse, child_orders, coupling_rows
):
    inverse = child_inverse[0]
    coupling = coupling_block[0]
    coupling_index = coupling_rows[0]
    columns = child_rhs.shape[2]
    child_order = inverse.shape[1]
    block_rows = root_rhs.shape[0]
    root_order = root_inverse.shape[1] * lax.axis_size("src")
    alive = (lax.iota(jnp.int32, child_order) < child_orders[0])[:, None]
    child_source = jnp.where(alive, child_rhs[0], 0.0).astype(jnp.bfloat16)
    forward = jnp.dot(
        lax.all_gather(inverse, "src", axis=0, tiled=True),
        child_source,
        preferred_element_type=jnp.float32,
    )
    child_solved = jnp.where(alive, forward, 0.0)
    solved_round = child_solved.astype(jnp.bfloat16)
    update = jnp.dot(
        lax.all_gather(coupling, "src", axis=0, tiled=True),
        solved_round,
        preferred_element_type=jnp.float32,
    )
    placed = jnp.zeros((root_order, columns), jnp.float32).at[coupling_index].add(update)
    first_row = lax.axis_index("sub") * block_rows
    own_rows = lax.dynamic_slice_in_dim(placed, first_row, block_rows, 0)
    summand = lax.dynamic_update_slice_in_dim(-placed, root_rhs - own_rows, first_row, 0)
    root_source = lax.psum(summand, "sub").astype(jnp.bfloat16)
    root_forward = jnp.dot(
        lax.all_gather(root_inverse, "src", axis=1, tiled=True),
        root_source,
        preferred_element_type=jnp.float32,
    )
    root_round = root_forward.astype(jnp.bfloat16)
    partial_root = contract_rows(
        lax.all_gather(root_inverse, "src", axis=1, tiled=True), root_round
    )
    root_out = lax.psum_scatter(partial_root, "sub", scatter_dimension=0, tiled=True)
    rounded_all = lax.all_gather(root_out.astype(jnp.bfloat16), "sub", axis=0, tiled=True)
    picked = rounded_all[coupling_index]
    pulled = contract_rows(lax.all_gather(coupling, "src", axis=0, tiled=True), picked)
    residue = jnp.where(alive, child_solved - pulled, 0.0).astype(jnp.bfloat16)
    backward = contract_rows(lax.all_gather(inverse, "src", axis=0, tiled=True), residue)
    child_out = jnp.where(alive, backward, 0.0)[None]
    return (child_out, root_out)


def route(child_rhs, root_rhs, child_inverse, *rest):
    n, subs = lax.axis_size("src"), lax.axis_size("sub")
    order = child_inverse.shape[2]
    fits = subs == 2 and n % 4 == 0 and n >= 8 and root_rhs.shape[0] == order == rest[0].shape[1] * n
    width, part = rest[1].shape[1], order // 4
    fits = fits and width == 128 and part % width == 0 and part * n % order == 0
    fits = fits and child_rhs.shape[2] == 2 * width
    form = fused if fits else on_device
    return form(child_rhs, root_rhs, child_inverse, *rest)


def solution(mesh):
    return jax.shard_map(
        route,
        mesh=mesh,
        in_specs=(
            P("sub", None, "src"),
            P("sub", "src"),
            P("sub", "src", None),
            P("sub", "src", None),
            P("sub", "src"),
            P("sub"),
            P("sub", None),
        ),
        out_specs=(P("sub", None, "src"), P("sub", "src")),
        check_vma=False,
    )
```

```python
import functools
import jax
import jax.numpy as jnp
from jax import lax
from jax.experimental import pallas as pl
from jax.experimental.pallas import tpu as pltpu
from jax.sharding import PartitionSpec as P

MESH = pl.DeviceIdType.MESH
F32 = jnp.float32
BF16 = jnp.bfloat16

INV, CPL, LAST, B2, B1, B0, CROSS = range(7)


def dot_t(left, right):
    return lax.dot_general(left, right, (((1,), (1,)), ((), ())), preferred_element_type=F32)


def dot_n(left, right):
    return jnp.dot(left, right, preferred_element_type=F32)


def kernel(
    lines, rhs_any, rrhs_any, inv_ref, cpl_ref, rinv_ref, order_ref, rows_ref, child_out, root_out,
    inv, cpl, root, hot, hott, column, rows_peer, rhs_ref, rrhs_ref,
    src_t, solved_t, upd_t, upd_peer, rr_give, rr_take, base_t, take, rr_t, sol_t, sol_b, res_t,
    recv, send_z, send_y, send_x, send_c, early_s, rows_r, rr_r, up_s, up_r, bk_s, bk_r, lay,
):
    me, x = lax.axis_index("src"), lax.axis_index("sub")
    core, y, z = me % 2, (me // 2) % 2, me // 4
    strip = inv_ref.shape[0]
    order = inv_ref.shape[1]
    width = rinv_ref.shape[1]
    part = root.shape[1]
    chunks = root.shape[0]
    per = rinv_ref.shape[0] // part
    block = 2 * part
    cols = rhs_ref.shape[1]
    hcols = cols // 2
    own_rows = rrhs_ref.shape[0]
    here = pl.multiple_of(x * hcols, hcols)
    there = pl.multiple_of((1 - x) * hcols, hcols)

    def src_of(zz, yy, cc):
        return (zz * 2 + yy) * 2 + cc

    def dev(zz, yy, cc, xx):
        return {"src": src_of(zz, yy, cc), "sub": xx}

    loads = [
        pltpu.make_async_copy(rhs_any, rhs_ref, lay.at[0]),
        pltpu.make_async_copy(rrhs_any, rrhs_ref, lay.at[1]),
    ]
    for copy in loads:
        copy.start()

    barrier = pltpu.get_barrier_semaphore()

    def hello(device):
        pl.semaphore_signal(barrier, inc=1, device_id=device, device_id_type=MESH)

    hello(dev(z, 1 - y, core, x))
    hello(dev(z, y, 1 - core, x))
    hello(dev(z, y, core, 1 - x))

    def greet(zz, _):
        pl.when(zz != z)(lambda: hello(dev(zz, y, core, x)))
        return 0
    lax.fori_loop(0, lines, greet, 0)

    def strip_ref(which, s):
        r = pl.multiple_of(s * strip, strip)
        return (inv if which == INV else cpl).at[pl.ds(r, strip), :]

    def cols_of(s):
        return pl.ds(pl.multiple_of(s * width, width), width)

    def chunk_ref(k, s):
        return root.at[k, :, cols_of(s)]

    placing = [
        pltpu.make_async_copy(inv_ref, strip_ref(INV, me), lay.at[2]),
        pltpu.make_async_copy(cpl_ref, strip_ref(CPL, me), lay.at[3]),
    ] + [
        pltpu.make_async_copy(
            rinv_ref.at[pl.ds(i * part, part), :], chunk_ref(per * x + i, me), lay.at[4 + i]
        )
        for i in range(per)
    ]
    for copy in placing:
        copy.start()

    last = chunks - 2 + x
    cross = chunks - 1 - x
    native_of = {B2: x == 1, B1: x == 0, B0: x == 0, LAST: x == 1}
    block_of = {B2: 2, B1: 1, B0: 0}

    def views(which, s):
        if which == INV:
            r = pl.multiple_of(s * strip, strip)
            return [
                (s * strip // part == q, inv.at[pl.ds(r, strip), pl.ds(0, (q + 1) * part)])
                for q in range(order // part)
            ]
        if which == CPL:
            return [(None, strip_ref(CPL, s))]
        if which in (LAST, CROSS):
            k = last if which == LAST else cross
            return [(s * width < (k + 1) * part, chunk_ref(k, s))]
        b = block_of[which]
        full = s * width < b * block + part
        some = jnp.logical_and(s * width >= b * block + part, s * width < (b + 1) * block)
        return [
            (full, root.at[pl.ds(2 * b, 2), :, cols_of(s)]),
            (some, chunk_ref(2 * b + 1, s)),
        ]

    def under(cond, f):
        if cond is None:
            f()
        else:
            pl.when(cond)(f)

    def rsem(which, s):
        if which == LAST:
            return recv.at[LAST + x, s]
        if which == CROSS:
            return recv.at[LAST + 1 - x, s]
        return recv.at[which if which < LAST else which + 1, s]

    def push(which, s, sem, device, wait=False):
        for cond, ref in views(which, s):
            def f(ref=ref):
                cp = pltpu.make_async_remote_copy(
                    src_ref=ref, dst_ref=ref, send_sem=sem, recv_sem=rsem(which, s),
                    device_id=device, device_id_type=MESH,
                )
                if wait:
                    cp.wait_send()
                else:
                    cp.start()
            under(cond, f)

    def arrive(which, s):
        for cond, ref in views(which, s):
            def f(ref=ref):
                pltpu.make_async_remote_copy(
                    src_ref=ref, dst_ref=ref, send_sem=recv.at[0, 0], recv_sem=rsem(which, s),
                    device_id=dev(z, y, 1 - core, x), device_id_type=MESH,
                ).wait_recv()
            under(cond, f)

    other = dev(z, y, core, 1 - x)

    def sends(which, zz, far, wait):
        yy = 1 - y if far else y
        s = src_of(zz, yy, core)
        if not far or which == LAST:
            @pl.when(jnp.logical_and(zz <= z, z < lines - 1))
            def _():
                push(which, s, send_z.at[which, int(far), 0, zz], dev(z + 1, y, core, x), wait)

            @pl.when(jnp.logical_and(zz >= z, z > 0))
            def _():
                push(which, s, send_z.at[which, int(far), 1, zz], dev(z - 1, y, core, x), wait)
        if not far:
            under(
                zz == z if which == LAST else None,
                lambda: push(which, s, send_y.at[which, zz], dev(z, 1 - y, core, x), wait),
            )
        if which == LAST:
            wanted = jnp.logical_or(zz != z, x == 1) if not far else None
            under(wanted, lambda: push(which, s, send_x.at[int(far), zz], other, wait))
        push(which, s, send_c.at[which, int(far), zz], dev(z, y, 1 - core, x), wait)

    def own(which):
        if which in native_of:
            pl.when(jnp.logical_not(native_of[which]))(lambda: arrive(which, me))
        sends(which, z, False, False)

    def either(d, f):
        def step(k, _):
            zz = z + d * (2 * k - 1)
            pl.when(jnp.logical_and(zz >= 0, zz < lines))(lambda: f(zz))
            return 0
        lax.fori_loop(0, 2, step, 0)

    def near(which, *distances):
        def one(zz):
            for away in (False, True) if which == LAST else (False,):
                arrive(which, src_of(zz, 1 - y if away else y, core))
                sends(which, zz, away, False)
        for d in distances:
            either(d, one)

    def far(which, *distances):
        def one(zz):
            arrive(which, src_of(zz, 1 - y, core))
            sends(which, zz, True, False)
        for d in distances:
            one(z) if d == 0 else either(d, one)

    def over_core(which):
        def step(k, _):
            arrive(which, src_of(k // 2, k % 2, 1 - core))
            return 0
        lax.fori_loop(0, 2 * lines, step, 0)

    def crossed():
        def step(k, _):
            s = src_of(k // 2, k % 2, core)

            @pl.when(jnp.logical_or(s != me, x == 0))
            def _():
                arrive(CROSS, s)
                push(CROSS, s, send_c.at[CROSS, k % 2, k // 2], dev(z, y, 1 - core, x))
            return 0
        lax.fori_loop(0, 2 * lines, step, 0)

    def cross_own(wait):
        @pl.when(x == 1)
        def _():
            push(CROSS, me, send_c.at[CROSS, y, z], dev(z, y, 1 - core, x), wait)

    def early(wait):
        def one(which, i):
            push(which, me, early_s.at[i], other, wait)

        @pl.when(x == 1)
        def _():
            one(CROSS, 0)
            one(B2, 1)

        @pl.when(x == 0)
        def _():
            one(B1, 2)
            one(B0, 3)

    def copy_rows():
        return pltpu.make_async_remote_copy(
            src_ref=rows_ref, dst_ref=rows_peer, send_sem=early_s.at[4], recv_sem=rows_r,
            device_id=other, device_id_type=MESH,
        )

    def copy_rrhs():
        return pltpu.make_async_remote_copy(
            src_ref=rr_give, dst_ref=rr_take, send_sem=early_s.at[5], recv_sem=rr_r,
            device_id=other, device_id_type=MESH,
        )

    def copy_update():
        return pltpu.make_async_remote_copy(
            src_ref=upd_t.at[pl.ds(there, hcols), :], dst_ref=upd_peer, send_sem=up_s,
            recv_sem=up_r, device_id=other, device_id_type=MESH,
        )

    def back(a):
        piece = sol_b.at[pl.ds(here, hcols), pl.ds(a * block, block)]
        return pltpu.make_async_remote_copy(
            src_ref=piece, dst_ref=piece, send_sem=bk_s.at[a], recv_sem=bk_r.at[a],
            device_id=other, device_id_type=MESH,
        )

    def turn(slot, index):
        column[slot] = jnp.broadcast_to(index, (width, order)).T

    def scatter_ones(slot):
        @pl.loop(0, order // width)
        def _(i):
            r = pl.multiple_of(i * width, width)
            at = column[slot, pl.ds(r, width), :]
            lane = lax.broadcasted_iota(jnp.int32, (width, width), 1)
            for t in range(hott.shape[2] // width):
                hott[slot, pl.ds(r, width), pl.ds(t * width, width)] = jnp.where(
                    at == lane + t * width, 1.0, 0.0
                ).astype(BF16)

    def gather_ones(index):
        @pl.loop(0, hot.shape[0] // part)
        def _(i):
            r = pl.multiple_of(i * part, part)
            at = lax.broadcasted_iota(jnp.int32, (part, order), 0) + r
            hot[pl.ds(r, part), :] = jnp.where(at == index, 1.0, 0.0).astype(BF16)

    pl.semaphore_wait(barrier, lines + 2)
    for copy in placing:
        copy.wait()

    own(INV)
    early(False)
    copy_rows().start()
    own(CPL)
    cross_own(False)
    pl.when(x == 1)(lambda: own(LAST))
    for copy in loads:
        copy.wait()
    rr_give[...] = rrhs_ref[:, pl.ds(there, hcols)].T.astype(BF16)
    copy_rrhs().start()
    pl.when(x == 0)(lambda: own(LAST))
    near(INV, 1)
    alive = lax.broadcasted_iota(jnp.int32, (1, order), 1) < order_ref[0]
    src_t[...] = jnp.where(alive, rhs_ref[...].T, 0.0).astype(BF16)
    near(CPL, 1)
    near(INV, 2)
    far(LAST, 0)
    far(INV, 0)
    own(B2)
    near(LAST, 1)
    near(CPL, 2)
    near(INV, *range(3, lines))
    far(INV, 1)
    far(CPL, 0)
    own(B1)
    near(B2, 1)
    near(LAST, 2)
    near(CPL, *range(3, lines))
    far(INV, *range(2, lines))
    far(CPL, 1)
    own(B0)
    index = rows_ref[...]
    turn(0, index)
    scatter_ones(0)
    over_core(INV)
    near(B1, 1)
    near(B2, 2)
    near(LAST, *range(3, lines))
    for q in range(order // part):
        at = pl.ds(q * part, part)
        upto = pl.ds(0, (q + 1) * part)
        solved_t[:, at] = jnp.where(
            alive[:, q * part:(q + 1) * part], dot_t(src_t[:, upto], inv[at, upto]), 0.0
        )
    far(CPL, *range(2, lines))
    near(B0, 1)
    near(B1, 2)
    near(B2, *range(3, lines))
    over_core(CPL)
    upd_t[...] = dot_t(solved_t[...].astype(BF16), cpl[...]).astype(BF16)
    copy_update().start()
    far(B2, 0, 1)
    near(B0, 2)
    near(B1, *range(3, lines))
    mine = pl.ds(pl.multiple_of(x * own_rows, own_rows), own_rows)
    theirs = pl.ds(pl.multiple_of((1 - x) * own_rows, own_rows), own_rows)
    copy_rrhs().wait_recv()
    base_t[:, mine] = rrhs_ref[:, pl.ds(here, hcols)].T
    base_t[:, theirs] = rr_take[...].astype(F32)
    mine_upd = upd_t[pl.ds(here, hcols), :]
    for i in range(hott.shape[2] // block):
        at = pl.ds(i * block, block)
        base_t[:, at] = base_t[:, at] - dot_n(mine_upd, hott[0, :, at])
    near(B0, *range(3, lines))
    copy_rows().wait_recv()
    turn(1, rows_peer[...])
    scatter_ones(1)
    crossed()
    far(B2, *range(2, lines))
    over_core(LAST)
    gather_ones(index)
    over_core(CROSS)
    far(B1, 0, 1)
    copy_update().wait_recv()
    for i in range(hott.shape[2] // block):
        at = pl.ds(i * block, block)
        take[:, at] = (base_t[:, at] - dot_n(upd_peer[...], hott[1, :, at])).astype(BF16)

    blocks = chunks // 2
    for b in reversed(range(blocks)):
        if b < blocks - 1:
            if b == 1:
                far(B1, *range(2, lines))
            if b == 0:
                far(B0, *range(lines))
            over_core((B0, B1, B2)[b])
        for k in (2 * b + 1, 2 * b):
            upto = pl.ds(0, (k + 1) * part)
            rr_t[:, pl.ds(k * part, part)] = dot_t(take[:, upto], root[k, :, upto]).astype(BF16)
        low, high = 2 * b, 2 * b + 1
        r_low, r_high = rr_t[:, pl.ds(low * part, part)], rr_t[:, pl.ds(high * part, part)]
        at_low, at_high = pl.ds(low * part, part), pl.ds(high * part, part)
        s_low = dot_n(r_low, root[low, :, at_low]) + dot_n(r_high, root[high, :, at_low])
        s_high = dot_n(r_high, root[high, :, at_high])
        if b < blocks - 1:
            s_low += sol_t[:, at_low]
            s_high += sol_t[:, at_high]
        sol_t[:, at_low] = s_low
        sol_t[:, at_high] = s_high
        sol_b[pl.ds(here, hcols), at_low] = s_low.astype(BF16)
        sol_b[pl.ds(here, hcols), at_high] = s_high.astype(BF16)
        if b < blocks - 1:
            back(b + 1).start()
        for a in reversed(range(b)):
            at = pl.ds(a * block, block)
            more = dot_n(r_low, root[low, :, at]) + dot_n(r_high, root[high, :, at])
            sol_t[:, at] = more if b == blocks - 1 else sol_t[:, at] + more
    back(0).start()

    def finish(first, picked):
        rows = pl.ds(first, hcols)
        pulled = dot_n(picked.astype(BF16), cpl[...])
        res_t[...] = jnp.where(alive, solved_t[rows, :] - pulled, 0.0).astype(BF16)
        for q in range(order // part):
            at, rest = pl.ds(q * part, part), pl.ds(q * part, order - q * part)
            solved = jnp.where(
                alive[:, q * part:(q + 1) * part], dot_n(res_t[:, rest], inv[rest, at]), 0.0
            )
            child_out[at, rows] = solved.T

    finish(here, dot_n(sol_b[pl.ds(here, hcols), :], hot[...]))
    root_out[:, pl.ds(here, hcols)] = sol_t[:, mine].T
    for a in range(1, blocks):
        back(a).wait_recv()
    upper = pl.ds(block, (blocks - 1) * block)
    picked = dot_n(sol_b[pl.ds(there, hcols), upper], hot[upper, :])
    back(0).wait_recv()
    lower = pl.ds(0, block)
    picked += dot_n(sol_b[pl.ds(there, hcols), lower], hot[lower, :])
    finish(there, picked)
    root_out[:, pl.ds(there, hcols)] = sol_b[pl.ds(there, hcols), mine].astype(F32).T

    early(True)
    cross_own(True)
    copy_rows().wait_send()
    copy_rrhs().wait_send()
    copy_update().wait_send()
    for a in range(blocks):
        back(a).wait_send()
    for which in (INV, CPL, LAST, B2, B1, B0):
        for away in (False, True):
            def step(zz, _, which=which, away=away):
                sends(which, zz, away, True)
                return 0
            lax.fori_loop(0, lines, step, 0)

    def step(k, _):
        s = src_of(k // 2, k % 2, core)

        @pl.when(jnp.logical_or(s != me, x == 0))
        def _():
            push(CROSS, s, send_c.at[CROSS, k % 2, k // 2], dev(z, y, 1 - core, x), True)
        return 0
    lax.fori_loop(0, 2 * lines, step, 0)


def fused(child_rhs, root_rhs, child_inverse, coupling_block, root_inverse, child_orders, coupling_rows):
    n = lax.axis_size("src")
    lines = n // 4
    order = child_inverse.shape[2]
    cols = child_rhs.shape[2]
    own_rows = root_rhs.shape[0]
    root_order = own_rows * lax.axis_size("sub")
    couples = coupling_block.shape[1] * n
    part = root_order // 8
    width = root_inverse.shape[1]
    half = cols // 2
    vmem = pl.BlockSpec(memory_space=pltpu.VMEM)
    smem = pl.BlockSpec(memory_space=pltpu.SMEM)
    anywhere = pl.BlockSpec(memory_space=pl.ANY)
    dma = pltpu.SemaphoreType.DMA
    child_out, root_out = pl.pallas_call(
        functools.partial(kernel, lines),
        out_shape=(
            pltpu.VMEM((order, cols), F32),
            pltpu.VMEM((own_rows, cols), F32),
        ),
        in_specs=[anywhere] * 2 + [vmem] * 3 + [smem, vmem],
        out_specs=(vmem, vmem),
        scratch_shapes=[
            pltpu.VMEM((order, order), BF16),
            pltpu.VMEM((couples, order), BF16),
            pltpu.VMEM((8, part, root_order), BF16),
            pltpu.VMEM((root_order, couples), BF16),
            pltpu.VMEM((2, couples, root_order), BF16),
            pltpu.VMEM((2, couples, width), jnp.int32),
            pltpu.VMEM((1, couples), jnp.int32),
            pltpu.VMEM((order, cols), F32),
            pltpu.VMEM((own_rows, cols), F32),
            pltpu.VMEM((cols, order), BF16),
            pltpu.VMEM((cols, order), F32),
            pltpu.VMEM((cols, couples), BF16),
            pltpu.VMEM((half, couples), BF16),
            pltpu.VMEM((half, own_rows), BF16),
            pltpu.VMEM((half, own_rows), BF16),
            pltpu.VMEM((half, root_order), F32),
            pltpu.VMEM((half, root_order), BF16),
            pltpu.VMEM((half, root_order), BF16),
            pltpu.VMEM((half, root_order), F32),
            pltpu.VMEM((cols, root_order), BF16),
            pltpu.VMEM((half, order), BF16),
            dma((7, n)),
            dma((6, 2, 2, lines)),
            dma((6, lines)),
            dma((2, lines)),
            dma((7, 2, lines)),
            dma((6,)),
            dma,
            dma,
            dma,
            dma,
            dma((4,)),
            dma((4,)),
            dma((8,)),
        ],
        compiler_params=pltpu.CompilerParams(
            collective_id=0, has_side_effects=True, vmem_limit_bytes=60 * 1024 * 1024
        ),
    )(child_rhs[0], root_rhs, child_inverse[0], coupling_block[0], root_inverse, child_orders, coupling_rows)
    return child_out[None], root_out


def contract_rows(left, right):
    return lax.dot_general(
        left, right, (((0,), (0,)), ((), ())), preferred_element_type=jnp.float32
    )


def on_device(
    child_rhs, root_rhs, child_inverse, coupling_block, root_inverse, child_orders, coupling_rows
):
    inverse = child_inverse[0]
    coupling = coupling_block[0]
    coupling_index = coupling_rows[0]
    columns = child_rhs.shape[2]
    child_order = inverse.shape[1]
    block_rows = root_rhs.shape[0]
    root_order = root_inverse.shape[1] * lax.axis_size("src")
    alive = (lax.iota(jnp.int32, child_order) < child_orders[0])[:, None]
    child_source = jnp.where(alive, child_rhs[0], 0.0).astype(jnp.bfloat16)
    forward = jnp.dot(
        lax.all_gather(inverse, "src", axis=0, tiled=True),
        child_source,
        preferred_element_type=jnp.float32,
    )
    child_solved = jnp.where(alive, forward, 0.0)
    solved_round = child_solved.astype(jnp.bfloat16)
    update = jnp.dot(
        lax.all_gather(coupling, "src", axis=0, tiled=True),
        solved_round,
        preferred_element_type=jnp.float32,
    )
    placed = jnp.zeros((root_order, columns), jnp.float32).at[coupling_index].add(update)
    first_row = lax.axis_index("sub") * block_rows
    own_rows = lax.dynamic_slice_in_dim(placed, first_row, block_rows, 0)
    summand = lax.dynamic_update_slice_in_dim(-placed, root_rhs - own_rows, first_row, 0)
    root_source = lax.psum(summand, "sub").astype(jnp.bfloat16)
    root_forward = jnp.dot(
        lax.all_gather(root_inverse, "src", axis=1, tiled=True),
        root_source,
        preferred_element_type=jnp.float32,
    )
    root_round = root_forward.astype(jnp.bfloat16)
    partial_root = contract_rows(
        lax.all_gather(root_inverse, "src", axis=1, tiled=True), root_round
    )
    root_out = lax.psum_scatter(partial_root, "sub", scatter_dimension=0, tiled=True)
    rounded_all = lax.all_gather(root_out.astype(jnp.bfloat16), "sub", axis=0, tiled=True)
    picked = rounded_all[coupling_index]
    pulled = contract_rows(lax.all_gather(coupling, "src", axis=0, tiled=True), picked)
    residue = jnp.where(alive, child_solved - pulled, 0.0).astype(jnp.bfloat16)
    backward = contract_rows(lax.all_gather(inverse, "src", axis=0, tiled=True), residue)
    child_out = jnp.where(alive, backward, 0.0)[None]
    return (child_out, root_out)


def route(child_rhs, root_rhs, child_inverse, *rest):
    n, subs = lax.axis_size("src"), lax.axis_size("sub")
    order = child_inverse.shape[2]
    fits = subs == 2 and n % 4 == 0 and n >= 8 and root_rhs.shape[0] == order == rest[0].shape[1] * n
    width, part = rest[1].shape[1], order // 4
    fits = fits and width == 128 and part % width == 0 and part * n % order == 0
    fits = fits and child_rhs.shape[2] == 2 * width
    form = fused if fits else on_device
    return form(child_rhs, root_rhs, child_inverse, *rest)


def solution(mesh):
    return jax.shard_map(
        route,
        mesh=mesh,
        in_specs=(
            P("sub", None, "src"),
            P("sub", "src"),
            P("sub", "src", None),
            P("sub", "src", None),
            P("sub", "src"),
            P("sub"),
            P("sub", None),
        ),
        out_specs=(P("sub", None, "src"), P("sub", "src")),
        check_vma=False,
    )
```

```python
import functools
import jax
import jax.numpy as jnp
from jax import lax
from jax.experimental import pallas as pl
from jax.experimental.pallas import tpu as pltpu
from jax.sharding import PartitionSpec as P

MESH = pl.DeviceIdType.MESH
F32 = jnp.float32
BF16 = jnp.bfloat16

INV, CPL, LAST, B2, B1, B0, CROSS = range(7)


def dot_t(left, right):
    return lax.dot_general(left, right, (((1,), (1,)), ((), ())), preferred_element_type=F32)


def dot_n(left, right):
    return jnp.dot(left, right, preferred_element_type=F32)


def kernel(
    lines, rhs_any, rrhs_any, inv_ref, cpl_ref, rinv_ref, order_ref, rows_any, child_out, root_out,
    inv, cpl, root, hot, hott, column, rows_ref, rows_peer, rhs_ref, rrhs_ref,
    src_t, solved_t, upd_t, upd_peer, rr_give, rr_take, base_t, take, rr_t, sol_t, sol_b, res_t,
    recv, send_z, send_y, send_x, send_c, early_s, rows_r, rr_r, up_s, up_r, bk_s, bk_r, lay,
):
    me, x = lax.axis_index("src"), lax.axis_index("sub")
    core, y, z = me % 2, (me // 2) % 2, me // 4
    strip = inv_ref.shape[0]
    order = inv_ref.shape[1]
    width = rinv_ref.shape[1]
    part = root.shape[1]
    chunks = root.shape[0]
    per = rinv_ref.shape[0] // part
    block = 2 * part
    cols = rhs_ref.shape[1]
    hcols = cols // 2
    own_rows = rrhs_ref.shape[0]
    here = pl.multiple_of(x * hcols, hcols)
    there = pl.multiple_of((1 - x) * hcols, hcols)

    def src_of(zz, yy, cc):
        return (zz * 2 + yy) * 2 + cc

    def dev(zz, yy, cc, xx):
        return {"src": src_of(zz, yy, cc), "sub": xx}

    barrier = pltpu.get_barrier_semaphore()

    def hello(device):
        pl.semaphore_signal(barrier, inc=1, device_id=device, device_id_type=MESH)

    hello(dev(z, 1 - y, core, x))
    hello(dev(z, y, 1 - core, x))
    hello(dev(z, y, core, 1 - x))

    def greet(zz, _):
        pl.when(zz != z)(lambda: hello(dev(zz, y, core, x)))
        return 0
    lax.fori_loop(0, lines, greet, 0)

    loads = [
        pltpu.make_async_copy(rhs_any, rhs_ref, lay.at[0]),
        pltpu.make_async_copy(rrhs_any, rrhs_ref, lay.at[1]),
        pltpu.make_async_copy(rows_any, rows_ref, lay.at[8]),
    ]

    def strip_ref(which, s):
        r = pl.multiple_of(s * strip, strip)
        return (inv if which == INV else cpl).at[pl.ds(r, strip), :]

    def cols_of(s):
        return pl.ds(pl.multiple_of(s * width, width), width)

    def chunk_ref(k, s):
        return root.at[k, :, cols_of(s)]

    placing = [
        pltpu.make_async_copy(inv_ref, strip_ref(INV, me), lay.at[2]),
        pltpu.make_async_copy(cpl_ref, strip_ref(CPL, me), lay.at[3]),
    ] + [
        pltpu.make_async_copy(
            rinv_ref.at[pl.ds(i * part, part), :], chunk_ref(per * x + i, me), lay.at[4 + i]
        )
        for i in range(per)
    ]
    for copy in placing + loads:
        copy.start()

    last = chunks - 2 + x
    cross = chunks - 1 - x
    native_of = {B2: x == 1, B1: x == 0, B0: x == 0, LAST: x == 1}
    block_of = {B2: 2, B1: 1, B0: 0}

    def views(which, s):
        if which == INV:
            r = pl.multiple_of(s * strip, strip)
            return [
                (s * strip // part == q, inv.at[pl.ds(r, strip), pl.ds(0, (q + 1) * part)])
                for q in range(order // part)
            ]
        if which == CPL:
            return [(None, strip_ref(CPL, s))]
        if which in (LAST, CROSS):
            k = last if which == LAST else cross
            return [(s * width < (k + 1) * part, chunk_ref(k, s))]
        b = block_of[which]
        full = s * width < b * block + part
        some = jnp.logical_and(s * width >= b * block + part, s * width < (b + 1) * block)
        return [
            (full, root.at[pl.ds(2 * b, 2), :, cols_of(s)]),
            (some, chunk_ref(2 * b + 1, s)),
        ]

    def under(cond, f):
        if cond is None:
            f()
        else:
            pl.when(cond)(f)

    def rsem(which, s):
        if which == LAST:
            return recv.at[LAST + x, s]
        if which == CROSS:
            return recv.at[LAST + 1 - x, s]
        return recv.at[which if which < LAST else which + 1, s]

    def push(which, s, sem, device, wait=False):
        for cond, ref in views(which, s):
            def f(ref=ref):
                cp = pltpu.make_async_remote_copy(
                    src_ref=ref, dst_ref=ref, send_sem=sem, recv_sem=rsem(which, s),
                    device_id=device, device_id_type=MESH,
                )
                if wait:
                    cp.wait_send()
                else:
                    cp.start()
            under(cond, f)

    def arrive(which, s):
        for cond, ref in views(which, s):
            def f(ref=ref):
                pltpu.make_async_remote_copy(
                    src_ref=ref, dst_ref=ref, send_sem=recv.at[0, 0], recv_sem=rsem(which, s),
                    device_id=dev(z, y, 1 - core, x), device_id_type=MESH,
                ).wait_recv()
            under(cond, f)

    other = dev(z, y, core, 1 - x)

    def sends(which, zz, far, wait):
        yy = 1 - y if far else y
        s = src_of(zz, yy, core)
        if not far or which == LAST:
            @pl.when(jnp.logical_and(zz <= z, z < lines - 1))
            def _():
                push(which, s, send_z.at[which, int(far), 0, zz], dev(z + 1, y, core, x), wait)

            @pl.when(jnp.logical_and(zz >= z, z > 0))
            def _():
                push(which, s, send_z.at[which, int(far), 1, zz], dev(z - 1, y, core, x), wait)
        if not far:
            under(
                zz == z if which == LAST else None,
                lambda: push(which, s, send_y.at[which, zz], dev(z, 1 - y, core, x), wait),
            )
        if which == LAST:
            wanted = jnp.logical_or(zz != z, x == 1) if not far else None
            under(wanted, lambda: push(which, s, send_x.at[int(far), zz], other, wait))
        push(which, s, send_c.at[which, int(far), zz], dev(z, y, 1 - core, x), wait)

    def own(which):
        if which in native_of:
            pl.when(jnp.logical_not(native_of[which]))(lambda: arrive(which, me))
        sends(which, z, False, False)

    def either(d, f):
        def step(k, _):
            zz = z + d * (2 * k - 1)
            pl.when(jnp.logical_and(zz >= 0, zz < lines))(lambda: f(zz))
            return 0
        lax.fori_loop(0, 2, step, 0)

    def near(which, *distances):
        def one(zz):
            for away in (False, True) if which == LAST else (False,):
                arrive(which, src_of(zz, 1 - y if away else y, core))
                sends(which, zz, away, False)
        for d in distances:
            either(d, one)

    def far(which, *distances):
        def one(zz):
            arrive(which, src_of(zz, 1 - y, core))
            sends(which, zz, True, False)
        for d in distances:
            one(z) if d == 0 else either(d, one)

    def over_core(which):
        def step(k, _):
            arrive(which, src_of(k // 2, k % 2, 1 - core))
            return 0
        lax.fori_loop(0, 2 * lines, step, 0)

    def crossed():
        def step(k, _):
            s = src_of(k // 2, k % 2, core)

            @pl.when(jnp.logical_or(s != me, x == 0))
            def _():
                arrive(CROSS, s)
                push(CROSS, s, send_c.at[CROSS, k % 2, k // 2], dev(z, y, 1 - core, x))
            return 0
        lax.fori_loop(0, 2 * lines, step, 0)

    def cross_own(wait):
        @pl.when(x == 1)
        def _():
            push(CROSS, me, send_c.at[CROSS, y, z], dev(z, y, 1 - core, x), wait)

    def early(wait):
        def one(which, i):
            push(which, me, early_s.at[i], other, wait)

        @pl.when(x == 1)
        def _():
            one(CROSS, 0)
            one(B2, 1)

        @pl.when(x == 0)
        def _():
            one(B1, 2)
            one(B0, 3)

    def copy_rows():
        return pltpu.make_async_remote_copy(
            src_ref=rows_ref, dst_ref=rows_peer, send_sem=early_s.at[4], recv_sem=rows_r,
            device_id=other, device_id_type=MESH,
        )

    def copy_rrhs():
        return pltpu.make_async_remote_copy(
            src_ref=rr_give, dst_ref=rr_take, send_sem=early_s.at[5], recv_sem=rr_r,
            device_id=other, device_id_type=MESH,
        )

    def copy_update():
        return pltpu.make_async_remote_copy(
            src_ref=upd_t.at[pl.ds(there, hcols), :], dst_ref=upd_peer, send_sem=up_s,
            recv_sem=up_r, device_id=other, device_id_type=MESH,
        )

    def back(a):
        piece = sol_b.at[pl.ds(here, hcols), pl.ds(a * block, block)]
        return pltpu.make_async_remote_copy(
            src_ref=piece, dst_ref=piece, send_sem=bk_s.at[a], recv_sem=bk_r.at[a],
            device_id=other, device_id_type=MESH,
        )

    def turn(slot, index):
        column[slot] = jnp.broadcast_to(index, (width, order)).T

    def scatter_ones(slot):
        @pl.loop(0, order // width)
        def _(i):
            r = pl.multiple_of(i * width, width)
            at = column[slot, pl.ds(r, width), :]
            lane = lax.broadcasted_iota(jnp.int32, (width, width), 1)
            for t in range(hott.shape[2] // width):
                hott[slot, pl.ds(r, width), pl.ds(t * width, width)] = jnp.where(
                    at == lane + t * width, 1.0, 0.0
                ).astype(BF16)

    def gather_ones(index):
        @pl.loop(0, hot.shape[0] // part)
        def _(i):
            r = pl.multiple_of(i * part, part)
            at = lax.broadcasted_iota(jnp.int32, (part, order), 0) + r
            hot[pl.ds(r, part), :] = jnp.where(at == index, 1.0, 0.0).astype(BF16)

    pl.semaphore_wait(barrier, lines + 2)
    for copy in placing:
        copy.wait()

    alive = lax.broadcasted_iota(jnp.int32, (1, order), 1) < order_ref[0]
    mine = pl.ds(pl.multiple_of(x * own_rows, own_rows), own_rows)
    theirs = pl.ds(pl.multiple_of((1 - x) * own_rows, own_rows), own_rows)
    blocks = chunks // 2

    def give_rhs():
        loads[1].wait()
        rr_give[...] = rrhs_ref[:, pl.ds(there, hcols)].T.astype(BF16)
        base_t[:, mine] = rrhs_ref[:, pl.ds(here, hcols)].T
        copy_rrhs().start()

    def source():
        loads[0].wait()
        src_t[...] = jnp.where(alive, rhs_ref[...].T, 0.0).astype(BF16)

    def ones(slot, index_ref):
        turn(slot, index_ref[...])
        scatter_ones(slot)

    def solve(q):
        at = pl.ds(q * part, part)
        upto = pl.ds(0, (q + 1) * part)
        solved_t[:, at] = jnp.where(
            alive[:, q * part:(q + 1) * part], dot_t(src_t[:, upto], inv[at, upto]), 0.0
        )

    def update():
        upd_t[...] = dot_t(solved_t[...].astype(BF16), cpl[...]).astype(BF16)
        copy_update().start()

    def scatter_mine():
        copy_rrhs().wait_recv()
        base_t[:, theirs] = rr_take[...].astype(F32)
        mine_upd = upd_t[pl.ds(here, hcols), :]
        for i in range(hott.shape[2] // block):
            at = pl.ds(i * block, block)
            base_t[:, at] = base_t[:, at] - dot_n(mine_upd, hott[0, :, at])

    def scatter_theirs():
        copy_update().wait_recv()
        for i in range(hott.shape[2] // block):
            at = pl.ds(i * block, block)
            take[:, at] = (base_t[:, at] - dot_n(upd_peer[...], hott[1, :, at])).astype(BF16)

    def root_block(b):
        for k in (2 * b + 1, 2 * b):
            upto = pl.ds(0, (k + 1) * part)
            rr_t[:, pl.ds(k * part, part)] = dot_t(take[:, upto], root[k, :, upto]).astype(BF16)
        low, high = 2 * b, 2 * b + 1
        r_low, r_high = rr_t[:, pl.ds(low * part, part)], rr_t[:, pl.ds(high * part, part)]
        at_low, at_high = pl.ds(low * part, part), pl.ds(high * part, part)
        s_low = dot_n(r_low, root[low, :, at_low]) + dot_n(r_high, root[high, :, at_low])
        s_high = dot_n(r_high, root[high, :, at_high])
        if b < blocks - 1:
            s_low += sol_t[:, at_low]
            s_high += sol_t[:, at_high]
        sol_t[:, at_low] = s_low
        sol_t[:, at_high] = s_high
        sol_b[pl.ds(here, hcols), at_low] = s_low.astype(BF16)
        sol_b[pl.ds(here, hcols), at_high] = s_high.astype(BF16)
        for a in reversed(range(b)):
            at = pl.ds(a * block, block)
            more = dot_n(r_low, root[low, :, at]) + dot_n(r_high, root[high, :, at])
            sol_t[:, at] = more if b == blocks - 1 else sol_t[:, at] + more
        back(b).start()

    own(INV)
    own(CPL)
    loads[2].wait()
    copy_rows().start()
    early(False)
    cross_own(False)
    pl.when(x == 0)(lambda: own(LAST))
    source()
    copy_rows().wait_recv()
    ones(1, rows_peer)
    near(INV, 1)
    pl.when(x == 1)(lambda: own(LAST))
    near(CPL, 1)
    near(INV, 2)
    give_rhs()
    own(B2)
    near(INV, 3)
    near(CPL, 2)
    far(INV, 0)
    far(LAST, 0)
    far(INV, 3, 2)
    near(CPL, 3)
    far(INV, 1)
    near(LAST, 1)
    far(CPL, 0)
    over_core(INV)
    far(CPL, 1)
    solve(0)
    near(LAST, 2)
    near(B2, 1)
    far(CPL, 2)
    own(B1)
    solve(3)
    solve(2)
    far(CPL, 3)
    near(LAST, 3)
    own(B0)
    over_core(CPL)
    far(B2, 0)
    solve(1)
    near(B2, 2)
    update()
    near(B1, 1)
    near(B2, 3)
    crossed()
    far(B2, 1)
    ones(0, rows_ref)
    scatter_mine()
    near(B1, 2, 3)
    far(B1, 0)
    far(B0, 0)
    over_core(LAST)
    scatter_theirs()
    far(B1, 2)
    far(B2, 2, 3)
    near(B0, 2, 1)
    over_core(CROSS)
    root_block(3)
    far(B1, 3)
    over_core(B2)
    far(B1, 1)
    root_block(2)
    near(B0, 3)
    over_core(B1)
    gather_ones(rows_ref[...])
    root_block(1)
    far(B0, 1, 3, 2)
    over_core(B0)
    root_block(0)

    def finish(first, picked):
        rows = pl.ds(first, hcols)
        pulled = dot_n(picked.astype(BF16), cpl[...])
        res_t[...] = jnp.where(alive, solved_t[rows, :] - pulled, 0.0).astype(BF16)
        for q in range(order // part):
            at, rest = pl.ds(q * part, part), pl.ds(q * part, order - q * part)
            solved = jnp.where(
                alive[:, q * part:(q + 1) * part], dot_n(res_t[:, rest], inv[rest, at]), 0.0
            )
            child_out[at, rows] = solved.T

    finish(here, dot_n(sol_b[pl.ds(here, hcols), :], hot[...]))
    root_out[:, pl.ds(here, hcols)] = sol_t[:, mine].T
    early(True)
    cross_own(True)
    copy_rows().wait_send()
    copy_rrhs().wait_send()
    copy_update().wait_send()
    for which in (INV, CPL, LAST, B2, B1, B0):
        for away in (False, True):
            def step(zz, _, which=which, away=away):
                sends(which, zz, away, True)
                return 0
            lax.fori_loop(0, lines, step, 0)

    def step(k, _):
        s = src_of(k // 2, k % 2, core)

        @pl.when(jnp.logical_or(s != me, x == 0))
        def _():
            push(CROSS, s, send_c.at[CROSS, k % 2, k // 2], dev(z, y, 1 - core, x), True)
        return 0
    lax.fori_loop(0, 2 * lines, step, 0)

    for a in range(1, blocks):
        back(a).wait_recv()
    upper = pl.ds(block, (blocks - 1) * block)
    picked = dot_n(sol_b[pl.ds(there, hcols), upper], hot[upper, :])
    back(0).wait_recv()
    lower = pl.ds(0, block)
    picked += dot_n(sol_b[pl.ds(there, hcols), lower], hot[lower, :])
    finish(there, picked)
    root_out[:, pl.ds(there, hcols)] = sol_b[pl.ds(there, hcols), mine].astype(F32).T
    for a in range(blocks):
        back(a).wait_send()


def fused(child_rhs, root_rhs, child_inverse, coupling_block, root_inverse, child_orders, coupling_rows):
    n = lax.axis_size("src")
    lines = n // 4
    order = child_inverse.shape[2]
    cols = child_rhs.shape[2]
    own_rows = root_rhs.shape[0]
    root_order = own_rows * lax.axis_size("sub")
    couples = coupling_block.shape[1] * n
    part = root_order // 8
    width = root_inverse.shape[1]
    half = cols // 2
    vmem = pl.BlockSpec(memory_space=pltpu.VMEM)
    smem = pl.BlockSpec(memory_space=pltpu.SMEM)
    anywhere = pl.BlockSpec(memory_space=pl.ANY)
    dma = pltpu.SemaphoreType.DMA
    child_out, root_out = pl.pallas_call(
        functools.partial(kernel, lines),
        out_shape=(
            pltpu.VMEM((order, cols), F32),
            pltpu.VMEM((own_rows, cols), F32),
        ),
        in_specs=[anywhere] * 5 + [smem, anywhere],
        out_specs=(vmem, vmem),
        scratch_shapes=[
            pltpu.VMEM((order, order), BF16),
            pltpu.VMEM((couples, order), BF16),
            pltpu.VMEM((8, part, root_order), BF16),
            pltpu.VMEM((root_order, couples), BF16),
            pltpu.VMEM((2, couples, root_order), BF16),
            pltpu.VMEM((2, couples, width), jnp.int32),
            pltpu.VMEM((1, couples), jnp.int32),
            pltpu.VMEM((1, couples), jnp.int32),
            pltpu.VMEM((order, cols), F32),
            pltpu.VMEM((own_rows, cols), F32),
            pltpu.VMEM((cols, order), BF16),
            pltpu.VMEM((cols, order), F32),
            pltpu.VMEM((cols, couples), BF16),
            pltpu.VMEM((half, couples), BF16),
            pltpu.VMEM((half, own_rows), BF16),
            pltpu.VMEM((half, own_rows), BF16),
            pltpu.VMEM((half, root_order), F32),
            pltpu.VMEM((half, root_order), BF16),
            pltpu.VMEM((half, root_order), BF16),
            pltpu.VMEM((half, root_order), F32),
            pltpu.VMEM((cols, root_order), BF16),
            pltpu.VMEM((half, order), BF16),
            dma((7, n)),
            dma((6, 2, 2, lines)),
            dma((6, lines)),
            dma((2, lines)),
            dma((7, 2, lines)),
            dma((6,)),
            dma,
            dma,
            dma,
            dma,
            dma((4,)),
            dma((4,)),
            dma((9,)),
        ],
        compiler_params=pltpu.CompilerParams(
            collective_id=0, has_side_effects=True, vmem_limit_bytes=60 * 1024 * 1024
        ),
    )(child_rhs[0], root_rhs, child_inverse[0], coupling_block[0], root_inverse, child_orders, coupling_rows)
    return child_out[None], root_out


def contract_rows(left, right):
    return lax.dot_general(
        left, right, (((0,), (0,)), ((), ())), preferred_element_type=jnp.float32
    )


def on_device(
    child_rhs, root_rhs, child_inverse, coupling_block, root_inverse, child_orders, coupling_rows
):
    inverse = child_inverse[0]
    coupling = coupling_block[0]
    coupling_index = coupling_rows[0]
    columns = child_rhs.shape[2]
    child_order = inverse.shape[1]
    block_rows = root_rhs.shape[0]
    root_order = root_inverse.shape[1] * lax.axis_size("src")
    alive = (lax.iota(jnp.int32, child_order) < child_orders[0])[:, None]
    child_source = jnp.where(alive, child_rhs[0], 0.0).astype(jnp.bfloat16)
    forward = jnp.dot(
        lax.all_gather(inverse, "src", axis=0, tiled=True),
        child_source,
        preferred_element_type=jnp.float32,
    )
    child_solved = jnp.where(alive, forward, 0.0)
    solved_round = child_solved.astype(jnp.bfloat16)
    update = jnp.dot(
        lax.all_gather(coupling, "src", axis=0, tiled=True),
        solved_round,
        preferred_element_type=jnp.float32,
    )
    placed = jnp.zeros((root_order, columns), jnp.float32).at[coupling_index].add(update)
    first_row = lax.axis_index("sub") * block_rows
    own_rows = lax.dynamic_slice_in_dim(placed, first_row, block_rows, 0)
    summand = lax.dynamic_update_slice_in_dim(-placed, root_rhs - own_rows, first_row, 0)
    root_source = lax.psum(summand, "sub").astype(jnp.bfloat16)
    root_forward = jnp.dot(
        lax.all_gather(root_inverse, "src", axis=1, tiled=True),
        root_source,
        preferred_element_type=jnp.float32,
    )
    root_round = root_forward.astype(jnp.bfloat16)
    partial_root = contract_rows(
        lax.all_gather(root_inverse, "src", axis=1, tiled=True), root_round
    )
    root_out = lax.psum_scatter(partial_root, "sub", scatter_dimension=0, tiled=True)
    rounded_all = lax.all_gather(root_out.astype(jnp.bfloat16), "sub", axis=0, tiled=True)
    picked = rounded_all[coupling_index]
    pulled = contract_rows(lax.all_gather(coupling, "src", axis=0, tiled=True), picked)
    residue = jnp.where(alive, child_solved - pulled, 0.0).astype(jnp.bfloat16)
    backward = contract_rows(lax.all_gather(inverse, "src", axis=0, tiled=True), residue)
    child_out = jnp.where(alive, backward, 0.0)[None]
    return (child_out, root_out)


def route(child_rhs, root_rhs, child_inverse, *rest):
    n, subs = lax.axis_size("src"), lax.axis_size("sub")
    order = child_inverse.shape[2]
    fits = subs == 2 and n % 4 == 0 and n >= 8 and root_rhs.shape[0] == order == rest[0].shape[1] * n
    width, part = rest[1].shape[1], order // 4
    fits = fits and width == 128 and part % width == 0 and part * n % order == 0
    fits = fits and child_rhs.shape[2] == 2 * width
    form = fused if fits else on_device
    return form(child_rhs, root_rhs, child_inverse, *rest)


def solution(mesh):
    return jax.shard_map(
        route,
        mesh=mesh,
        in_specs=(
            P("sub", None, "src"),
            P("sub", "src"),
            P("sub", "src", None),
            P("sub", "src", None),
            P("sub", "src"),
            P("sub"),
            P("sub", None),
        ),
        out_specs=(P("sub", None, "src"), P("sub", "src")),
        check_vma=False,
    )
```

```python
import functools
import jax
import jax.numpy as jnp
from jax import lax
from jax.experimental import pallas as pl
from jax.experimental.pallas import tpu as pltpu
from jax.sharding import PartitionSpec as P

MESH = pl.DeviceIdType.MESH
F32 = jnp.float32
BF16 = jnp.bfloat16

INV, CPL, LAST, B2, B1, B0, CROSS = range(7)


def dot_t(left, right):
    return lax.dot_general(left, right, (((1,), (1,)), ((), ())), preferred_element_type=F32)


def dot_n(left, right):
    return jnp.dot(left, right, preferred_element_type=F32)


def kernel(
    lines, rhs_any, rrhs_any, inv_ref, cpl_ref, rinv_ref, order_ref, rows_any, child_out, root_out,
    inv, cpl, root, hot, hott, column, rows_ref, rows_peer, rhs_ref, rrhs_ref,
    src_t, solved_t, upd_t, upd_peer, rr_give, rr_take, base_t, take, rr_t, sol_t, sol_b, res_t,
    recv, send_z, send_y, send_x, send_c, early_s, rows_r, rr_r, up_s, up_r, bk_s, bk_r, lay,
):
    me, x = lax.axis_index("src"), lax.axis_index("sub")
    core, y, z = me % 2, (me // 2) % 2, me // 4
    strip = inv_ref.shape[0]
    order = inv_ref.shape[1]
    width = rinv_ref.shape[1]
    part = root.shape[1]
    chunks = root.shape[0]
    per = rinv_ref.shape[0] // part
    block = 2 * part
    cols = rhs_ref.shape[1]
    hcols = cols // 2
    own_rows = rrhs_ref.shape[0]
    here = pl.multiple_of(x * hcols, hcols)
    there = pl.multiple_of((1 - x) * hcols, hcols)

    def src_of(zz, yy, cc):
        return (zz * 2 + yy) * 2 + cc

    def dev(zz, yy, cc, xx):
        return {"src": src_of(zz, yy, cc), "sub": xx}

    barrier = pltpu.get_barrier_semaphore()

    def hello(device):
        pl.semaphore_signal(barrier, inc=1, device_id=device, device_id_type=MESH)

    hello(dev(z, 1 - y, core, x))
    hello(dev(z, y, 1 - core, x))
    hello(dev(z, y, core, 1 - x))

    @pl.when(z > 0)
    def _():
        hello(dev(z - 1, y, core, x))

    @pl.when(z < lines - 1)
    def _():
        hello(dev(z + 1, y, core, x))

    loads = [
        pltpu.make_async_copy(rhs_any, rhs_ref, lay.at[0]),
        pltpu.make_async_copy(rrhs_any, rrhs_ref, lay.at[1]),
        pltpu.make_async_copy(rows_any, rows_ref, lay.at[8]),
    ]

    def strip_ref(which, s):
        r = pl.multiple_of(s * strip, strip)
        return (inv if which == INV else cpl).at[pl.ds(r, strip), :]

    def cols_of(s):
        return pl.ds(pl.multiple_of(s * width, width), width)

    def chunk_ref(k, s):
        return root.at[k, :, cols_of(s)]

    placing = [
        pltpu.make_async_copy(inv_ref, strip_ref(INV, me), lay.at[2]),
        pltpu.make_async_copy(cpl_ref, strip_ref(CPL, me), lay.at[3]),
    ] + [
        pltpu.make_async_copy(
            rinv_ref.at[pl.ds(i * part, part), :], chunk_ref(per * x + i, me), lay.at[4 + i]
        )
        for i in range(per)
    ]
    for copy in placing + loads:
        copy.start()

    last = chunks - 2 + x
    cross = chunks - 1 - x
    native_of = {B2: x == 1, B1: x == 0, B0: x == 0, LAST: x == 1}
    block_of = {B2: 2, B1: 1, B0: 0}

    def views(which, s):
        if which == INV:
            r = pl.multiple_of(s * strip, strip)
            return [
                (s * strip // part == q, inv.at[pl.ds(r, strip), pl.ds(0, (q + 1) * part)])
                for q in range(order // part)
            ]
        if which == CPL:
            return [(None, strip_ref(CPL, s))]
        if which in (LAST, CROSS):
            k = last if which == LAST else cross
            return [(s * width < (k + 1) * part, chunk_ref(k, s))]
        b = block_of[which]
        full = s * width < b * block + part
        some = jnp.logical_and(s * width >= b * block + part, s * width < (b + 1) * block)
        return [
            (full, root.at[pl.ds(2 * b, 2), :, cols_of(s)]),
            (some, chunk_ref(2 * b + 1, s)),
        ]

    def under(cond, f):
        if cond is None:
            f()
        else:
            pl.when(cond)(f)

    def rsem(which, s):
        if which == LAST:
            return recv.at[LAST + x, s]
        if which == CROSS:
            return recv.at[LAST + 1 - x, s]
        return recv.at[which if which < LAST else which + 1, s]

    def push(which, s, sem, device, wait=False):
        for cond, ref in views(which, s):
            def f(ref=ref):
                cp = pltpu.make_async_remote_copy(
                    src_ref=ref, dst_ref=ref, send_sem=sem, recv_sem=rsem(which, s),
                    device_id=device, device_id_type=MESH,
                )
                if wait:
                    cp.wait_send()
                else:
                    cp.start()
            under(cond, f)

    def arrive(which, s):
        for cond, ref in views(which, s):
            def f(ref=ref):
                pltpu.make_async_remote_copy(
                    src_ref=ref, dst_ref=ref, send_sem=recv.at[0, 0], recv_sem=rsem(which, s),
                    device_id=dev(z, y, 1 - core, x), device_id_type=MESH,
                ).wait_recv()
            under(cond, f)

    other = dev(z, y, core, 1 - x)

    def sends(which, zz, far, wait):
        yy = 1 - y if far else y
        s = src_of(zz, yy, core)
        if not far or which == LAST:
            @pl.when(jnp.logical_and(zz <= z, z < lines - 1))
            def _():
                push(which, s, send_z.at[which, int(far), 0, zz], dev(z + 1, y, core, x), wait)

            @pl.when(jnp.logical_and(zz >= z, z > 0))
            def _():
                push(which, s, send_z.at[which, int(far), 1, zz], dev(z - 1, y, core, x), wait)
        if not far:
            under(
                zz == z if which == LAST else None,
                lambda: push(which, s, send_y.at[which, zz], dev(z, 1 - y, core, x), wait),
            )
        if which == LAST:
            wanted = jnp.logical_or(zz != z, x == 1) if not far else None
            under(wanted, lambda: push(which, s, send_x.at[int(far), zz], other, wait))
        push(which, s, send_c.at[which, int(far), zz], dev(z, y, 1 - core, x), wait)

    def own(which):
        if which in native_of:
            pl.when(jnp.logical_not(native_of[which]))(lambda: arrive(which, me))
        sends(which, z, False, False)

    def either(d, f):
        def step(k, _):
            zz = z + d * (2 * k - 1)
            pl.when(jnp.logical_and(zz >= 0, zz < lines))(lambda: f(zz))
            return 0
        lax.fori_loop(0, 2, step, 0)

    def near(which, *distances):
        def one(zz):
            for away in (False, True) if which == LAST else (False,):
                arrive(which, src_of(zz, 1 - y if away else y, core))
                sends(which, zz, away, False)
        for d in distances:
            either(d, one)

    def far(which, *distances):
        def one(zz):
            arrive(which, src_of(zz, 1 - y, core))
            sends(which, zz, True, False)
        for d in distances:
            one(z) if d == 0 else either(d, one)

    def over_core(which):
        def step(k, _):
            arrive(which, src_of(k // 2, k % 2, 1 - core))
            return 0
        lax.fori_loop(0, 2 * lines, step, 0)

    def crossed():
        def step(k, _):
            s = src_of(k // 2, k % 2, core)

            @pl.when(jnp.logical_or(s != me, x == 0))
            def _():
                arrive(CROSS, s)
                push(CROSS, s, send_c.at[CROSS, k % 2, k // 2], dev(z, y, 1 - core, x))
            return 0
        lax.fori_loop(0, 2 * lines, step, 0)

    def cross_own(wait):
        @pl.when(x == 1)
        def _():
            push(CROSS, me, send_c.at[CROSS, y, z], dev(z, y, 1 - core, x), wait)

    def early(wait):
        def one(which, i):
            push(which, me, early_s.at[i], other, wait)

        @pl.when(x == 1)
        def _():
            one(CROSS, 0)
            one(B2, 1)

        @pl.when(x == 0)
        def _():
            one(B1, 2)
            one(B0, 3)

    def copy_rows():
        return pltpu.make_async_remote_copy(
            src_ref=rows_ref, dst_ref=rows_peer, send_sem=early_s.at[4], recv_sem=rows_r,
            device_id=other, device_id_type=MESH,
        )

    def copy_rrhs():
        return pltpu.make_async_remote_copy(
            src_ref=rr_give, dst_ref=rr_take, send_sem=early_s.at[5], recv_sem=rr_r,
            device_id=other, device_id_type=MESH,
        )

    def copy_update():
        return pltpu.make_async_remote_copy(
            src_ref=upd_t.at[pl.ds(there, hcols), :], dst_ref=upd_peer, send_sem=up_s,
            recv_sem=up_r, device_id=other, device_id_type=MESH,
        )

    def back(a):
        piece = sol_b.at[pl.ds(here, hcols), pl.ds(a * block, block)]
        return pltpu.make_async_remote_copy(
            src_ref=piece, dst_ref=piece, send_sem=bk_s.at[a], recv_sem=bk_r.at[a],
            device_id=other, device_id_type=MESH,
        )

    def turn(slot, index):
        column[slot] = jnp.broadcast_to(index, (width, order)).T

    def scatter_ones(slot):
        @pl.loop(0, order // width)
        def _(i):
            r = pl.multiple_of(i * width, width)
            at = column[slot, pl.ds(r, width), :]
            lane = lax.broadcasted_iota(jnp.int32, (width, width), 1)
            for t in range(hott.shape[2] // width):
                hott[slot, pl.ds(r, width), pl.ds(t * width, width)] = jnp.where(
                    at == lane + t * width, 1.0, 0.0
                ).astype(BF16)

    def gather_ones(index):
        @pl.loop(0, hot.shape[0] // part)
        def _(i):
            r = pl.multiple_of(i * part, part)
            at = lax.broadcasted_iota(jnp.int32, (part, order), 0) + r
            hot[pl.ds(r, part), :] = jnp.where(at == index, 1.0, 0.0).astype(BF16)

    inner = jnp.logical_and(z > 0, z < lines - 1)
    pl.when(inner)(lambda: pl.semaphore_wait(barrier, 5))
    pl.when(jnp.logical_not(inner))(lambda: pl.semaphore_wait(barrier, 4))
    for copy in placing:
        copy.wait()

    alive = lax.broadcasted_iota(jnp.int32, (1, order), 1) < order_ref[0]
    mine = pl.ds(pl.multiple_of(x * own_rows, own_rows), own_rows)
    theirs = pl.ds(pl.multiple_of((1 - x) * own_rows, own_rows), own_rows)
    blocks = chunks // 2

    def give_rhs():
        loads[1].wait()
        rr_give[...] = rrhs_ref[:, pl.ds(there, hcols)].T.astype(BF16)
        base_t[:, mine] = rrhs_ref[:, pl.ds(here, hcols)].T
        copy_rrhs().start()

    def source():
        loads[0].wait()
        src_t[...] = jnp.where(alive, rhs_ref[...].T, 0.0).astype(BF16)

    def ones(slot, index_ref):
        turn(slot, index_ref[...])
        scatter_ones(slot)

    def solve(q):
        at = pl.ds(q * part, part)
        upto = pl.ds(0, (q + 1) * part)
        solved_t[:, at] = jnp.where(
            alive[:, q * part:(q + 1) * part], dot_t(src_t[:, upto], inv[at, upto]), 0.0
        )

    def update():
        upd_t[...] = dot_t(solved_t[...].astype(BF16), cpl[...]).astype(BF16)
        copy_update().start()

    def scatter_mine():
        copy_rrhs().wait_recv()
        base_t[:, theirs] = rr_take[...].astype(F32)
        mine_upd = upd_t[pl.ds(here, hcols), :]
        for i in range(hott.shape[2] // block):
            at = pl.ds(i * block, block)
            base_t[:, at] = base_t[:, at] - dot_n(mine_upd, hott[0, :, at])

    def scatter_theirs():
        copy_update().wait_recv()
        for i in range(hott.shape[2] // block):
            at = pl.ds(i * block, block)
            take[:, at] = (base_t[:, at] - dot_n(upd_peer[...], hott[1, :, at])).astype(BF16)

    def root_block(b):
        for k in (2 * b + 1, 2 * b):
            upto = pl.ds(0, (k + 1) * part)
            rr_t[:, pl.ds(k * part, part)] = dot_t(take[:, upto], root[k, :, upto]).astype(BF16)
        low, high = 2 * b, 2 * b + 1
        r_low, r_high = rr_t[:, pl.ds(low * part, part)], rr_t[:, pl.ds(high * part, part)]
        at_low, at_high = pl.ds(low * part, part), pl.ds(high * part, part)
        s_low = dot_n(r_low, root[low, :, at_low]) + dot_n(r_high, root[high, :, at_low])
        s_high = dot_n(r_high, root[high, :, at_high])
        if b < blocks - 1:
            s_low += sol_t[:, at_low]
            s_high += sol_t[:, at_high]
        sol_t[:, at_low] = s_low
        sol_t[:, at_high] = s_high
        sol_b[pl.ds(here, hcols), at_low] = s_low.astype(BF16)
        sol_b[pl.ds(here, hcols), at_high] = s_high.astype(BF16)
        for a in reversed(range(b)):
            at = pl.ds(a * block, block)
            more = dot_n(r_low, root[low, :, at]) + dot_n(r_high, root[high, :, at])
            sol_t[:, at] = more if b == blocks - 1 else sol_t[:, at] + more
        back(b).start()

    own(INV)
    own(CPL)
    loads[2].wait()
    copy_rows().start()
    early(False)
    cross_own(False)
    pl.when(x == 0)(lambda: own(LAST))
    source()
    copy_rows().wait_recv()
    ones(1, rows_peer)
    near(INV, 1)
    pl.when(x == 1)(lambda: own(LAST))
    near(CPL, 1)
    near(INV, 2)
    give_rhs()
    own(B2)
    near(INV, 3)
    near(CPL, 2)
    far(INV, 0)
    far(LAST, 0)
    far(INV, 3, 2)
    near(CPL, 3)
    far(INV, 1)
    near(LAST, 1)
    far(CPL, 0)
    over_core(INV)
    far(CPL, 1)
    solve(0)
    near(LAST, 2)
    near(B2, 1)
    far(CPL, 2)
    own(B1)
    solve(3)
    solve(2)
    far(CPL, 3)
    near(LAST, 3)
    own(B0)
    over_core(CPL)
    far(B2, 0)
    solve(1)
    near(B2, 2)
    update()
    near(B1, 1)
    near(B2, 3)
    crossed()
    far(B2, 1)
    ones(0, rows_ref)
    scatter_mine()
    near(B1, 2, 3)
    far(B1, 0)
    far(B0, 0)
    over_core(LAST)
    scatter_theirs()
    far(B1, 2)
    far(B2, 2, 3)
    near(B0, 2, 1)
    over_core(CROSS)
    root_block(3)
    far(B1, 3)
    over_core(B2)
    far(B1, 1)
    root_block(2)
    near(B0, 3)
    over_core(B1)
    gather_ones(rows_ref[...])
    root_block(1)
    far(B0, 1, 3, 2)
    over_core(B0)
    root_block(0)

    def finish(first, picked):
        rows = pl.ds(first, hcols)
        pulled = dot_n(picked.astype(BF16), cpl[...])
        res_t[...] = jnp.where(alive, solved_t[rows, :] - pulled, 0.0).astype(BF16)
        for q in range(order // part):
            at, rest = pl.ds(q * part, part), pl.ds(q * part, order - q * part)
            solved = jnp.where(
                alive[:, q * part:(q + 1) * part], dot_n(res_t[:, rest], inv[rest, at]), 0.0
            )
            child_out[at, rows] = solved.T

    finish(here, dot_n(sol_b[pl.ds(here, hcols), :], hot[...]))
    root_out[:, pl.ds(here, hcols)] = sol_t[:, mine].T
    early(True)
    cross_own(True)
    copy_rows().wait_send()
    copy_rrhs().wait_send()
    copy_update().wait_send()
    for which in (INV, CPL, LAST, B2, B1, B0):
        for away in (False, True):
            def step(zz, _, which=which, away=away):
                sends(which, zz, away, True)
                return 0
            lax.fori_loop(0, lines, step, 0)

    def step(k, _):
        s = src_of(k // 2, k % 2, core)

        @pl.when(jnp.logical_or(s != me, x == 0))
        def _():
            push(CROSS, s, send_c.at[CROSS, k % 2, k // 2], dev(z, y, 1 - core, x), True)
        return 0
    lax.fori_loop(0, 2 * lines, step, 0)

    for a in range(1, blocks):
        back(a).wait_recv()
    upper = pl.ds(block, (blocks - 1) * block)
    picked = dot_n(sol_b[pl.ds(there, hcols), upper], hot[upper, :])
    back(0).wait_recv()
    lower = pl.ds(0, block)
    picked += dot_n(sol_b[pl.ds(there, hcols), lower], hot[lower, :])
    finish(there, picked)
    root_out[:, pl.ds(there, hcols)] = sol_b[pl.ds(there, hcols), mine].astype(F32).T
    for a in range(blocks):
        back(a).wait_send()


def fused(child_rhs, root_rhs, child_inverse, coupling_block, root_inverse, child_orders, coupling_rows):
    n = lax.axis_size("src")
    lines = n // 4
    order = child_inverse.shape[2]
    cols = child_rhs.shape[2]
    own_rows = root_rhs.shape[0]
    root_order = own_rows * lax.axis_size("sub")
    couples = coupling_block.shape[1] * n
    part = root_order // 8
    width = root_inverse.shape[1]
    half = cols // 2
    vmem = pl.BlockSpec(memory_space=pltpu.VMEM)
    smem = pl.BlockSpec(memory_space=pltpu.SMEM)
    anywhere = pl.BlockSpec(memory_space=pl.ANY)
    dma = pltpu.SemaphoreType.DMA
    child_out, root_out = pl.pallas_call(
        functools.partial(kernel, lines),
        out_shape=(
            pltpu.VMEM((order, cols), F32),
            pltpu.VMEM((own_rows, cols), F32),
        ),
        in_specs=[anywhere] * 5 + [smem, anywhere],
        out_specs=(vmem, vmem),
        scratch_shapes=[
            pltpu.VMEM((order, order), BF16),
            pltpu.VMEM((couples, order), BF16),
            pltpu.VMEM((8, part, root_order), BF16),
            pltpu.VMEM((root_order, couples), BF16),
            pltpu.VMEM((2, couples, root_order), BF16),
            pltpu.VMEM((2, couples, width), jnp.int32),
            pltpu.VMEM((1, couples), jnp.int32),
            pltpu.VMEM((1, couples), jnp.int32),
            pltpu.VMEM((order, cols), F32),
            pltpu.VMEM((own_rows, cols), F32),
            pltpu.VMEM((cols, order), BF16),
            pltpu.VMEM((cols, order), F32),
            pltpu.VMEM((cols, couples), BF16),
            pltpu.VMEM((half, couples), BF16),
            pltpu.VMEM((half, own_rows), BF16),
            pltpu.VMEM((half, own_rows), BF16),
            pltpu.VMEM((half, root_order), F32),
            pltpu.VMEM((half, root_order), BF16),
            pltpu.VMEM((half, root_order), BF16),
            pltpu.VMEM((half, root_order), F32),
            pltpu.VMEM((cols, root_order), BF16),
            pltpu.VMEM((half, order), BF16),
            dma((7, n)),
            dma((6, 2, 2, lines)),
            dma((6, lines)),
            dma((2, lines)),
            dma((7, 2, lines)),
            dma((6,)),
            dma,
            dma,
            dma,
            dma,
            dma((4,)),
            dma((4,)),
            dma((9,)),
        ],
        compiler_params=pltpu.CompilerParams(
            collective_id=0, has_side_effects=True, vmem_limit_bytes=60 * 1024 * 1024
        ),
    )(child_rhs[0], root_rhs, child_inverse[0], coupling_block[0], root_inverse, child_orders, coupling_rows)
    return child_out[None], root_out


def contract_rows(left, right):
    return lax.dot_general(
        left, right, (((0,), (0,)), ((), ())), preferred_element_type=jnp.float32
    )


def on_device(
    child_rhs, root_rhs, child_inverse, coupling_block, root_inverse, child_orders, coupling_rows
):
    inverse = child_inverse[0]
    coupling = coupling_block[0]
    coupling_index = coupling_rows[0]
    columns = child_rhs.shape[2]
    child_order = inverse.shape[1]
    block_rows = root_rhs.shape[0]
    root_order = root_inverse.shape[1] * lax.axis_size("src")
    alive = (lax.iota(jnp.int32, child_order) < child_orders[0])[:, None]
    child_source = jnp.where(alive, child_rhs[0], 0.0).astype(jnp.bfloat16)
    forward = jnp.dot(
        lax.all_gather(inverse, "src", axis=0, tiled=True),
        child_source,
        preferred_element_type=jnp.float32,
    )
    child_solved = jnp.where(alive, forward, 0.0)
    solved_round = child_solved.astype(jnp.bfloat16)
    update = jnp.dot(
        lax.all_gather(coupling, "src", axis=0, tiled=True),
        solved_round,
        preferred_element_type=jnp.float32,
    )
    placed = jnp.zeros((root_order, columns), jnp.float32).at[coupling_index].add(update)
    first_row = lax.axis_index("sub") * block_rows
    own_rows = lax.dynamic_slice_in_dim(placed, first_row, block_rows, 0)
    summand = lax.dynamic_update_slice_in_dim(-placed, root_rhs - own_rows, first_row, 0)
    root_source = lax.psum(summand, "sub").astype(jnp.bfloat16)
    root_forward = jnp.dot(
        lax.all_gather(root_inverse, "src", axis=1, tiled=True),
        root_source,
        preferred_element_type=jnp.float32,
    )
    root_round = root_forward.astype(jnp.bfloat16)
    partial_root = contract_rows(
        lax.all_gather(root_inverse, "src", axis=1, tiled=True), root_round
    )
    root_out = lax.psum_scatter(partial_root, "sub", scatter_dimension=0, tiled=True)
    rounded_all = lax.all_gather(root_out.astype(jnp.bfloat16), "sub", axis=0, tiled=True)
    picked = rounded_all[coupling_index]
    pulled = contract_rows(lax.all_gather(coupling, "src", axis=0, tiled=True), picked)
    residue = jnp.where(alive, child_solved - pulled, 0.0).astype(jnp.bfloat16)
    backward = contract_rows(lax.all_gather(inverse, "src", axis=0, tiled=True), residue)
    child_out = jnp.where(alive, backward, 0.0)[None]
    return (child_out, root_out)


def route(child_rhs, root_rhs, child_inverse, *rest):
    n, subs = lax.axis_size("src"), lax.axis_size("sub")
    order = child_inverse.shape[2]
    fits = subs == 2 and n % 4 == 0 and n >= 8 and root_rhs.shape[0] == order == rest[0].shape[1] * n
    width, part = rest[1].shape[1], order // 4
    fits = fits and width == 128 and part % width == 0 and part * n % order == 0
    fits = fits and child_rhs.shape[2] == 2 * width
    form = fused if fits else on_device
    return form(child_rhs, root_rhs, child_inverse, *rest)


def solution(mesh):
    return jax.shard_map(
        route,
        mesh=mesh,
        in_specs=(
            P("sub", None, "src"),
            P("sub", "src"),
            P("sub", "src", None),
            P("sub", "src", None),
            P("sub", "src"),
            P("sub"),
            P("sub", None),
        ),
        out_specs=(P("sub", None, "src"), P("sub", "src")),
        check_vma=False,
    )
```

```python
import functools
import jax
import jax.numpy as jnp
from jax import lax
from jax.experimental import pallas as pl
from jax.experimental.pallas import tpu as pltpu
from jax.sharding import PartitionSpec as P

MESH = pl.DeviceIdType.MESH
F32 = jnp.float32
BF16 = jnp.bfloat16

INV, CPL, LAST, B2, B1, B0, CROSS = range(7)


def dot_t(left, right):
    return lax.dot_general(left, right, (((1,), (1,)), ((), ())), preferred_element_type=F32)


def dot_n(left, right):
    return jnp.dot(left, right, preferred_element_type=F32)


def kernel(
    lines, rhs_any, rrhs_any, inv_ref, cpl_ref, rinv_ref, order_ref, rows_any, child_out, root_out,
    inv, cpl, root, hot, hott, column, rows_ref, rows_peer, rhs_ref, rrhs_ref,
    src_t, solved_t, upd_t, upd_peer, rr_give, rr_take, base_t, take, rr_t, sol_t, sol_b, res_t,
    recv, send_z, send_y, send_x, send_c, early_s, rows_r, rr_r, up_s, up_r, bk_s, bk_r, lay,
):
    me, x = lax.axis_index("src"), lax.axis_index("sub")
    core, y, z = me % 2, (me // 2) % 2, me // 4
    strip = inv_ref.shape[0]
    order = inv_ref.shape[1]
    width = rinv_ref.shape[1]
    part = root.shape[1]
    chunks = root.shape[0]
    per = rinv_ref.shape[0] // part
    block = 2 * part
    cols = rhs_ref.shape[1]
    hcols = cols // 2
    own_rows = rrhs_ref.shape[0]
    here = pl.multiple_of(x * hcols, hcols)
    there = pl.multiple_of((1 - x) * hcols, hcols)

    def src_of(zz, yy, cc):
        return (zz * 2 + yy) * 2 + cc

    def dev(zz, yy, cc, xx):
        return {"src": src_of(zz, yy, cc), "sub": xx}

    barrier = pltpu.get_barrier_semaphore()

    def hello(device):
        pl.semaphore_signal(barrier, inc=1, device_id=device, device_id_type=MESH)

    hello(dev(z, 1 - y, core, x))
    hello(dev(z, y, 1 - core, x))
    hello(dev(z, y, core, 1 - x))

    @pl.when(z > 0)
    def _():
        hello(dev(z - 1, y, core, x))

    @pl.when(z < lines - 1)
    def _():
        hello(dev(z + 1, y, core, x))

    loads = [
        pltpu.make_async_copy(rhs_any, rhs_ref, lay.at[0]),
        pltpu.make_async_copy(rrhs_any, rrhs_ref, lay.at[1]),
        pltpu.make_async_copy(rows_any, rows_ref, lay.at[8]),
    ]

    def strip_ref(which, s):
        r = pl.multiple_of(s * strip, strip)
        return (inv if which == INV else cpl).at[pl.ds(r, strip), :]

    def cols_of(s):
        return pl.ds(pl.multiple_of(s * width, width), width)

    def chunk_ref(k, s):
        return root.at[k, :, cols_of(s)]

    placing = [
        pltpu.make_async_copy(inv_ref, strip_ref(INV, me), lay.at[2]),
        pltpu.make_async_copy(cpl_ref, strip_ref(CPL, me), lay.at[3]),
    ] + [
        pltpu.make_async_copy(
            rinv_ref.at[pl.ds(i * part, part), :], chunk_ref(per * x + i, me), lay.at[4 + i]
        )
        for i in range(per)
    ]
    for copy in placing + loads:
        copy.start()

    last = chunks - 2 + x
    cross = chunks - 1 - x
    native_of = {B2: x == 1, B1: x == 0, B0: x == 0, LAST: x == 1}
    block_of = {B2: 2, B1: 1, B0: 0}

    def views(which, s):
        if which == INV:
            r = pl.multiple_of(s * strip, strip)
            return [
                (s * strip // part == q, inv.at[pl.ds(r, strip), pl.ds(0, (q + 1) * part)])
                for q in range(order // part)
            ]
        if which == CPL:
            return [(None, strip_ref(CPL, s))]
        if which in (LAST, CROSS):
            k = last if which == LAST else cross
            return [(s * width < (k + 1) * part, chunk_ref(k, s))]
        b = block_of[which]
        full = s * width < b * block + part
        some = jnp.logical_and(s * width >= b * block + part, s * width < (b + 1) * block)
        return [
            (full, root.at[pl.ds(2 * b, 2), :, cols_of(s)]),
            (some, chunk_ref(2 * b + 1, s)),
        ]

    def under(cond, f):
        if cond is None:
            f()
        else:
            pl.when(cond)(f)

    def rsem(which, s):
        if which == LAST:
            return recv.at[LAST + x, s]
        if which == CROSS:
            return recv.at[LAST + 1 - x, s]
        return recv.at[which if which < LAST else which + 1, s]

    def push(which, s, sem, device, wait=False):
        for cond, ref in views(which, s):
            def f(ref=ref):
                cp = pltpu.make_async_remote_copy(
                    src_ref=ref, dst_ref=ref, send_sem=sem, recv_sem=rsem(which, s),
                    device_id=device, device_id_type=MESH,
                )
                if wait:
                    cp.wait_send()
                else:
                    cp.start()
            under(cond, f)

    def arrive(which, s):
        for cond, ref in views(which, s):
            def f(ref=ref):
                pltpu.make_async_remote_copy(
                    src_ref=ref, dst_ref=ref, send_sem=recv.at[0, 0], recv_sem=rsem(which, s),
                    device_id=dev(z, y, 1 - core, x), device_id_type=MESH,
                ).wait_recv()
            under(cond, f)

    other = dev(z, y, core, 1 - x)

    def sends(which, zz, far, wait):
        yy = 1 - y if far else y
        s = src_of(zz, yy, core)
        if not far or which == LAST:
            @pl.when(jnp.logical_and(zz <= z, z < lines - 1))
            def _():
                push(which, s, send_z.at[which, int(far), 0, zz], dev(z + 1, y, core, x), wait)

            @pl.when(jnp.logical_and(zz >= z, z > 0))
            def _():
                push(which, s, send_z.at[which, int(far), 1, zz], dev(z - 1, y, core, x), wait)
        if not far:
            under(
                zz == z if which == LAST else None,
                lambda: push(which, s, send_y.at[which, zz], dev(z, 1 - y, core, x), wait),
            )
        if which == LAST:
            wanted = jnp.logical_or(zz != z, x == 1) if not far else None
            under(wanted, lambda: push(which, s, send_x.at[int(far), zz], other, wait))
        push(which, s, send_c.at[which, int(far), zz], dev(z, y, 1 - core, x), wait)

    def own(which):
        if which in native_of:
            pl.when(jnp.logical_not(native_of[which]))(lambda: arrive(which, me))
        sends(which, z, False, False)

    def either(d, f):
        def step(k, _):
            zz = z + d * (2 * k - 1)
            pl.when(jnp.logical_and(zz >= 0, zz < lines))(lambda: f(zz))
            return 0
        lax.fori_loop(0, 2, step, 0)

    def near(which, *distances):
        def one(zz):
            for away in (False, True) if which == LAST else (False,):
                arrive(which, src_of(zz, 1 - y if away else y, core))
                sends(which, zz, away, False)
        for d in distances:
            either(d, one)

    def far(which, *distances):
        def one(zz):
            arrive(which, src_of(zz, 1 - y, core))
            sends(which, zz, True, False)
        for d in distances:
            one(z) if d == 0 else either(d, one)

    def over_core(which):
        def step(k, _):
            arrive(which, src_of(k // 2, k % 2, 1 - core))
            return 0
        lax.fori_loop(0, 2 * lines, step, 0)

    def crossed():
        def step(k, _):
            s = src_of(k // 2, k % 2, core)

            @pl.when(jnp.logical_or(s != me, x == 0))
            def _():
                arrive(CROSS, s)
                push(CROSS, s, send_c.at[CROSS, k % 2, k // 2], dev(z, y, 1 - core, x))
            return 0
        lax.fori_loop(0, 2 * lines, step, 0)

    def cross_own(wait):
        @pl.when(x == 1)
        def _():
            push(CROSS, me, send_c.at[CROSS, y, z], dev(z, y, 1 - core, x), wait)

    def early(wait):
        def one(which, i):
            push(which, me, early_s.at[i], other, wait)

        @pl.when(x == 1)
        def _():
            one(CROSS, 0)
            one(B2, 1)

        @pl.when(x == 0)
        def _():
            one(B1, 2)
            one(B0, 3)

    def copy_rows():
        return pltpu.make_async_remote_copy(
            src_ref=rows_ref, dst_ref=rows_peer, send_sem=early_s.at[4], recv_sem=rows_r,
            device_id=other, device_id_type=MESH,
        )

    def copy_rrhs():
        return pltpu.make_async_remote_copy(
            src_ref=rr_give, dst_ref=rr_take, send_sem=early_s.at[5], recv_sem=rr_r,
            device_id=other, device_id_type=MESH,
        )

    def copy_update():
        return pltpu.make_async_remote_copy(
            src_ref=upd_t.at[pl.ds(there, hcols), :], dst_ref=upd_peer, send_sem=up_s,
            recv_sem=up_r, device_id=other, device_id_type=MESH,
        )

    def back(a):
        piece = sol_b.at[pl.ds(here, hcols), pl.ds(a * block, block)]
        return pltpu.make_async_remote_copy(
            src_ref=piece, dst_ref=piece, send_sem=bk_s.at[a], recv_sem=bk_r.at[a],
            device_id=other, device_id_type=MESH,
        )

    def turn(slot, index):
        column[slot] = jnp.broadcast_to(index, (width, order)).T

    def scatter_ones(slot):
        @pl.loop(0, order // width)
        def _(i):
            r = pl.multiple_of(i * width, width)
            at = column[slot, pl.ds(r, width), :]
            lane = lax.broadcasted_iota(jnp.int32, (width, width), 1)
            for t in range(hott.shape[2] // width):
                hott[slot, pl.ds(r, width), pl.ds(t * width, width)] = jnp.where(
                    at == lane + t * width, 1.0, 0.0
                ).astype(BF16)

    def gather_ones(index):
        @pl.loop(0, hot.shape[0] // part)
        def _(i):
            r = pl.multiple_of(i * part, part)
            at = lax.broadcasted_iota(jnp.int32, (part, order), 0) + r
            hot[pl.ds(r, part), :] = jnp.where(at == index, 1.0, 0.0).astype(BF16)

    inner = jnp.logical_and(z > 0, z < lines - 1)
    pl.when(inner)(lambda: pl.semaphore_wait(barrier, 5))
    pl.when(jnp.logical_not(inner))(lambda: pl.semaphore_wait(barrier, 4))
    placing[0].wait()

    alive = lax.broadcasted_iota(jnp.int32, (1, order), 1) < order_ref[0]
    mine = pl.ds(pl.multiple_of(x * own_rows, own_rows), own_rows)
    theirs = pl.ds(pl.multiple_of((1 - x) * own_rows, own_rows), own_rows)
    blocks = chunks // 2

    def give_rhs():
        loads[1].wait()
        rr_give[...] = rrhs_ref[:, pl.ds(there, hcols)].T.astype(BF16)
        base_t[:, mine] = rrhs_ref[:, pl.ds(here, hcols)].T
        copy_rrhs().start()

    def source():
        loads[0].wait()
        src_t[...] = jnp.where(alive, rhs_ref[...].T, 0.0).astype(BF16)

    def ones(slot, index_ref):
        turn(slot, index_ref[...])
        scatter_ones(slot)

    def solve(q):
        at = pl.ds(q * part, part)
        upto = pl.ds(0, (q + 1) * part)
        solved_t[:, at] = jnp.where(
            alive[:, q * part:(q + 1) * part], dot_t(src_t[:, upto], inv[at, upto]), 0.0
        )

    def update():
        upd_t[...] = dot_t(solved_t[...].astype(BF16), cpl[...]).astype(BF16)
        copy_update().start()

    def scatter_mine():
        copy_rrhs().wait_recv()
        base_t[:, theirs] = rr_take[...].astype(F32)
        mine_upd = upd_t[pl.ds(here, hcols), :]
        for i in range(hott.shape[2] // block):
            at = pl.ds(i * block, block)
            base_t[:, at] = base_t[:, at] - dot_n(mine_upd, hott[0, :, at])

    def scatter_theirs():
        copy_update().wait_recv()
        for i in range(hott.shape[2] // block):
            at = pl.ds(i * block, block)
            take[:, at] = (base_t[:, at] - dot_n(upd_peer[...], hott[1, :, at])).astype(BF16)

    def root_block(b):
        for k in (2 * b + 1, 2 * b):
            upto = pl.ds(0, (k + 1) * part)
            rr_t[:, pl.ds(k * part, part)] = dot_t(take[:, upto], root[k, :, upto]).astype(BF16)
        low, high = 2 * b, 2 * b + 1
        r_low, r_high = rr_t[:, pl.ds(low * part, part)], rr_t[:, pl.ds(high * part, part)]
        at_low, at_high = pl.ds(low * part, part), pl.ds(high * part, part)
        s_low = dot_n(r_low, root[low, :, at_low]) + dot_n(r_high, root[high, :, at_low])
        s_high = dot_n(r_high, root[high, :, at_high])
        if b < blocks - 1:
            s_low += sol_t[:, at_low]
            s_high += sol_t[:, at_high]
        sol_t[:, at_low] = s_low
        sol_t[:, at_high] = s_high
        sol_b[pl.ds(here, hcols), at_low] = s_low.astype(BF16)
        sol_b[pl.ds(here, hcols), at_high] = s_high.astype(BF16)
        for a in reversed(range(b)):
            at = pl.ds(a * block, block)
            more = dot_n(r_low, root[low, :, at]) + dot_n(r_high, root[high, :, at])
            sol_t[:, at] = more if b == blocks - 1 else sol_t[:, at] + more
        back(b).start()

    own(INV)
    placing[1].wait()
    own(CPL)
    for copy in placing[2:]:
        copy.wait()
    loads[2].wait()
    copy_rows().start()
    early(False)
    cross_own(False)
    pl.when(x == 0)(lambda: own(LAST))
    source()
    copy_rows().wait_recv()
    ones(1, rows_peer)
    near(INV, 1)
    pl.when(x == 1)(lambda: own(LAST))
    near(CPL, 1)
    near(INV, 2)
    give_rhs()
    own(B2)
    near(INV, 3)
    near(CPL, 2)
    far(INV, 0)
    far(LAST, 0)
    far(INV, 3, 2)
    near(CPL, 3)
    far(INV, 1)
    near(LAST, 1)
    far(CPL, 0)
    over_core(INV)
    far(CPL, 1)
    solve(0)
    near(LAST, 2)
    near(B2, 1)
    far(CPL, 2)
    own(B1)
    solve(3)
    solve(2)
    far(CPL, 3)
    near(LAST, 3)
    own(B0)
    over_core(CPL)
    far(B2, 0)
    solve(1)
    near(B2, 2)
    update()
    near(B1, 1)
    near(B2, 3)
    crossed()
    far(B2, 1)
    ones(0, rows_ref)
    scatter_mine()
    near(B1, 2, 3)
    far(B1, 0)
    far(B0, 0)
    over_core(LAST)
    scatter_theirs()
    far(B1, 2)
    far(B2, 2, 3)
    near(B0, 2, 1)
    over_core(CROSS)
    root_block(3)
    far(B1, 3)
    over_core(B2)
    far(B1, 1)
    root_block(2)
    near(B0, 3)
    over_core(B1)
    root_block(1)
    far(B0, 1, 3, 2)
    over_core(B0)
    root_block(0)

    gather_ones(rows_ref[...])

    def finish(first, picked):
        rows = pl.ds(first, hcols)
        pulled = dot_n(picked.astype(BF16), cpl[...])
        res_t[...] = jnp.where(alive, solved_t[rows, :] - pulled, 0.0).astype(BF16)
        for q in range(order // part):
            at, rest = pl.ds(q * part, part), pl.ds(q * part, order - q * part)
            solved = jnp.where(
                alive[:, q * part:(q + 1) * part], dot_n(res_t[:, rest], inv[rest, at]), 0.0
            )
            child_out[at, rows] = solved.T

    finish(here, dot_n(sol_b[pl.ds(here, hcols), :], hot[...]))
    root_out[:, pl.ds(here, hcols)] = sol_t[:, mine].T
    early(True)
    cross_own(True)
    copy_rows().wait_send()
    copy_rrhs().wait_send()
    copy_update().wait_send()
    for which in (INV, CPL, LAST, B2, B1, B0):
        for away in (False, True):
            def step(zz, _, which=which, away=away):
                sends(which, zz, away, True)
                return 0
            lax.fori_loop(0, lines, step, 0)

    def step(k, _):
        s = src_of(k // 2, k % 2, core)

        @pl.when(jnp.logical_or(s != me, x == 0))
        def _():
            push(CROSS, s, send_c.at[CROSS, k % 2, k // 2], dev(z, y, 1 - core, x), True)
        return 0
    lax.fori_loop(0, 2 * lines, step, 0)

    for a in range(1, blocks):
        back(a).wait_recv()
    upper = pl.ds(block, (blocks - 1) * block)
    picked = dot_n(sol_b[pl.ds(there, hcols), upper], hot[upper, :])
    back(0).wait_recv()
    lower = pl.ds(0, block)
    picked += dot_n(sol_b[pl.ds(there, hcols), lower], hot[lower, :])
    finish(there, picked)
    root_out[:, pl.ds(there, hcols)] = sol_b[pl.ds(there, hcols), mine].astype(F32).T
    for a in range(blocks):
        back(a).wait_send()


def fused(child_rhs, root_rhs, child_inverse, coupling_block, root_inverse, child_orders, coupling_rows):
    n = lax.axis_size("src")
    lines = n // 4
    order = child_inverse.shape[2]
    cols = child_rhs.shape[2]
    own_rows = root_rhs.shape[0]
    root_order = own_rows * lax.axis_size("sub")
    couples = coupling_block.shape[1] * n
    part = root_order // 8
    width = root_inverse.shape[1]
    half = cols // 2
    vmem = pl.BlockSpec(memory_space=pltpu.VMEM)
    smem = pl.BlockSpec(memory_space=pltpu.SMEM)
    anywhere = pl.BlockSpec(memory_space=pl.ANY)
    dma = pltpu.SemaphoreType.DMA
    child_out, root_out = pl.pallas_call(
        functools.partial(kernel, lines),
        out_shape=(
            pltpu.VMEM((order, cols), F32),
            pltpu.VMEM((own_rows, cols), F32),
        ),
        in_specs=[anywhere] * 5 + [smem, anywhere],
        out_specs=(vmem, vmem),
        scratch_shapes=[
            pltpu.VMEM((order, order), BF16),
            pltpu.VMEM((couples, order), BF16),
            pltpu.VMEM((8, part, root_order), BF16),
            pltpu.VMEM((root_order, couples), BF16),
            pltpu.VMEM((2, couples, root_order), BF16),
            pltpu.VMEM((2, couples, width), jnp.int32),
            pltpu.VMEM((1, couples), jnp.int32),
            pltpu.VMEM((1, couples), jnp.int32),
            pltpu.VMEM((order, cols), F32),
            pltpu.VMEM((own_rows, cols), F32),
            pltpu.VMEM((cols, order), BF16),
            pltpu.VMEM((cols, order), F32),
            pltpu.VMEM((cols, couples), BF16),
            pltpu.VMEM((half, couples), BF16),
            pltpu.VMEM((half, own_rows), BF16),
            pltpu.VMEM((half, own_rows), BF16),
            pltpu.VMEM((half, root_order), F32),
            pltpu.VMEM((half, root_order), BF16),
            pltpu.VMEM((half, root_order), BF16),
            pltpu.VMEM((half, root_order), F32),
            pltpu.VMEM((cols, root_order), BF16),
            pltpu.VMEM((half, order), BF16),
            dma((7, n)),
            dma((6, 2, 2, lines)),
            dma((6, lines)),
            dma((2, lines)),
            dma((7, 2, lines)),
            dma((6,)),
            dma,
            dma,
            dma,
            dma,
            dma((4,)),
            dma((4,)),
            dma((9,)),
        ],
        compiler_params=pltpu.CompilerParams(
            collective_id=0, has_side_effects=True, vmem_limit_bytes=60 * 1024 * 1024
        ),
    )(child_rhs[0], root_rhs, child_inverse[0], coupling_block[0], root_inverse, child_orders, coupling_rows)
    return child_out[None], root_out


def contract_rows(left, right):
    return lax.dot_general(
        left, right, (((0,), (0,)), ((), ())), preferred_element_type=jnp.float32
    )


def on_device(
    child_rhs, root_rhs, child_inverse, coupling_block, root_inverse, child_orders, coupling_rows
):
    inverse = child_inverse[0]
    coupling = coupling_block[0]
    coupling_index = coupling_rows[0]
    columns = child_rhs.shape[2]
    child_order = inverse.shape[1]
    block_rows = root_rhs.shape[0]
    root_order = root_inverse.shape[1] * lax.axis_size("src")
    alive = (lax.iota(jnp.int32, child_order) < child_orders[0])[:, None]
    child_source = jnp.where(alive, child_rhs[0], 0.0).astype(jnp.bfloat16)
    forward = jnp.dot(
        lax.all_gather(inverse, "src", axis=0, tiled=True),
        child_source,
        preferred_element_type=jnp.float32,
    )
    child_solved = jnp.where(alive, forward, 0.0)
    solved_round = child_solved.astype(jnp.bfloat16)
    update = jnp.dot(
        lax.all_gather(coupling, "src", axis=0, tiled=True),
        solved_round,
        preferred_element_type=jnp.float32,
    )
    placed = jnp.zeros((root_order, columns), jnp.float32).at[coupling_index].add(update)
    first_row = lax.axis_index("sub") * block_rows
    own_rows = lax.dynamic_slice_in_dim(placed, first_row, block_rows, 0)
    summand = lax.dynamic_update_slice_in_dim(-placed, root_rhs - own_rows, first_row, 0)
    root_source = lax.psum(summand, "sub").astype(jnp.bfloat16)
    root_forward = jnp.dot(
        lax.all_gather(root_inverse, "src", axis=1, tiled=True),
        root_source,
        preferred_element_type=jnp.float32,
    )
    root_round = root_forward.astype(jnp.bfloat16)
    partial_root = contract_rows(
        lax.all_gather(root_inverse, "src", axis=1, tiled=True), root_round
    )
    root_out = lax.psum_scatter(partial_root, "sub", scatter_dimension=0, tiled=True)
    rounded_all = lax.all_gather(root_out.astype(jnp.bfloat16), "sub", axis=0, tiled=True)
    picked = rounded_all[coupling_index]
    pulled = contract_rows(lax.all_gather(coupling, "src", axis=0, tiled=True), picked)
    residue = jnp.where(alive, child_solved - pulled, 0.0).astype(jnp.bfloat16)
    backward = contract_rows(lax.all_gather(inverse, "src", axis=0, tiled=True), residue)
    child_out = jnp.where(alive, backward, 0.0)[None]
    return (child_out, root_out)


def route(child_rhs, root_rhs, child_inverse, *rest):
    n, subs = lax.axis_size("src"), lax.axis_size("sub")
    order = child_inverse.shape[2]
    fits = subs == 2 and n % 4 == 0 and n >= 8 and root_rhs.shape[0] == order == rest[0].shape[1] * n
    width, part = rest[1].shape[1], order // 4
    fits = fits and width == 128 and part % width == 0 and part * n % order == 0
    fits = fits and child_rhs.shape[2] == 2 * width
    form = fused if fits else on_device
    return form(child_rhs, root_rhs, child_inverse, *rest)


def solution(mesh):
    return jax.shard_map(
        route,
        mesh=mesh,
        in_specs=(
            P("sub", None, "src"),
            P("sub", "src"),
            P("sub", "src", None),
            P("sub", "src", None),
            P("sub", "src"),
            P("sub"),
            P("sub", None),
        ),
        out_specs=(P("sub", None, "src"), P("sub", "src")),
        check_vma=False,
    )
```
